128 devices in a mesh: img: 16 (over y, z), pix: 8 (over x, core).
Axes of the slice: x: 4, y: 4, z: 4, core: 2. Of those that a mesh axis runs over, the one named last changes fastest.
Arguments:
- images: bfloat16 [6144, 16384], P('img', 'pix'), may hold values from -12 to 12
- inverse_noise_scale: float32 [6144], P('img'), may hold values from 0.4 to 4
- projections: bfloat16 [16384, 16384], P('img', 'pix'), may hold values from -1 to 1
- group_search_blocks: int32 [16, 16], P('img'), may hold values from 0 to 127, as said below
- search_list_count: int32 [16], P('img'), may hold values from 12 to 16, as said below
Outputs:
- projection_sums: float32 [16384, 16384], P('img', 'pix')
- log_evidence: float32 [6144], P(('img', 'pix'))
The draws below stay inside these ranges and needn't reach their ends.
Inputs may be any that keep to these rules, and one draw needn't show every extreme that they name: `group_search_blocks`: each row lists 16 different block ids; block b is owned by index b // 8 of img. Among the first search_list_count[g] entries of row g no owner appears more than 2 times, and in every draw one owner has 2 of its blocks among the first 2 entries of every row. `search_list_count`: some group's count is 16 in every draw.
All inputs are finite; a program needn't handle non-finite values.
Results may differ from the reference program's by a relative error of at most 0.004.
Values may be sent and summed in bfloat16 or wider, within the bound.
A program may use at most 128 MiB of HBM per device.

```python
import math
import jax
import jax.numpy as jnp
from jax import lax

F = 16384
BLOCK = 128
BLK_DEV = 8
CAP = 2
MAXL = 16
GROUP_IMAGES = 384
NBLK = 128
NPROJ = 16384
NIMG = 6144
N_IMG = 16


def search_table(key):
    base = jax.random.fold_in(key, 11)
    key_hot, key_order, key_offset, key_count, key_long = jax.random.split(base, 5)
    hot_owner = jax.random.randint(key_hot, (), 0, N_IMG)
    owner_orders = jax.vmap(lambda single: jax.random.permutation(single, N_IMG - 1))(jax.random.split(key_order, N_IMG))
    order_table = jnp.concatenate([jnp.full((N_IMG, 1), hot_owner, jnp.int32), ((hot_owner + 1 + owner_orders) % N_IMG).astype(jnp.int32)], axis=1)
    offset_table = jax.vmap(lambda single: jax.random.permutation(single, BLK_DEV)[:CAP])(jax.random.split(key_offset, N_IMG * N_IMG))
    offset_table = offset_table.reshape(N_IMG, N_IMG, CAP)
    positions = jnp.arange(MAXL)
    which_owner = positions // CAP
    inner_slot = positions % CAP
    owners = order_table[:, which_owner]
    offsets = offset_table[jnp.arange(N_IMG)[:, None], which_owner[None, :], inner_slot[None, :]]
    table = (owners * BLK_DEV + offsets).astype(jnp.int32)
    counts = MAXL - 4 + jax.random.randint(key_count, (N_IMG,), 0, 5)
    longest = jax.random.randint(key_long, (), 0, N_IMG)
    counts = jnp.where(jnp.arange(N_IMG) == longest, MAXL, counts).astype(jnp.int32)
    return (table, counts)


def projection_field(key):
    base = jax.random.fold_in(key, 12)
    key_main = jax.random.fold_in(base, 0)
    field = jax.random.normal(key_main, (NPROJ, F), jnp.float32) * F ** (-0.5)
    return jnp.clip(field, -12.0 * F ** (-0.5), 12.0 * F ** (-0.5))


def draw_group_search_blocks(key, part):
    return search_table(key)[0]


def draw_search_list_count(key, part):
    return search_table(key)[1]


def draw_projections(key, part):
    return projection_field(key).astype(jnp.bfloat16)


def draw_images(key, part):
    base = jax.random.fold_in(key, 13)
    key_main = jax.random.fold_in(base, 0)
    result = jax.random.normal(key_main, (NIMG, F), jnp.float32)
    return jnp.clip(result, -12.0, 12.0).astype(jnp.bfloat16)


def block_scale(key, extent, pieces, smallest, high):
    factor_of, own = 1.0, jax.random.fold_in(key, 6)
    for dim, parts in pieces:
        heights = jnp.exp(jax.random.uniform(jax.random.fold_in(own, dim), (parts,), jnp.float32, smallest / len(pieces), high / len(pieces)))
        factor_of = factor_of * jnp.repeat(heights, extent[dim] // parts).reshape([-1 if axis == dim else 1 for axis in range(len(extent))])
    return factor_of


def setup_inputs(seed: int = 0) -> dict:
    key_list = jax.random.split(jax.random.key(seed), 6)
    return {
        "images": draw_images(jax.random.fold_in(key_list[5], 71), 0),
        "inverse_noise_scale": jnp.clip(jnp.exp(math.log(4.0) - 2.3025851 * jax.random.uniform(key_list[1], (NIMG,), jnp.float32) ** block_scale(key_list[1], (NIMG,), ((0, 16),), -0.2, 0.2)), 0.4, 4.0),
        "projections": draw_projections(jax.random.fold_in(key_list[5], 71), 0),
        "group_search_blocks": draw_group_search_blocks(jax.random.fold_in(key_list[5], 71), 0),
        "search_list_count": draw_search_list_count(jax.random.fold_in(key_list[5], 71), 0),
    }


def reference(images, inverse_noise_scale, projections, group_search_blocks, search_list_count):
    blocks = projections.reshape(NBLK, BLOCK, F)
    images_by_group = images.reshape(N_IMG, GROUP_IMAGES, F)
    noise_scale_factors = inverse_noise_scale.reshape(N_IMG, GROUP_IMAGES)
    positions = jnp.arange(MAXL, dtype=jnp.int32)

    def visit_block(running_total, inputs):
        members, scaling, chosen, listed = inputs
        live_entry = positions < listed
        fetched = jnp.take(blocks, chosen.astype(jnp.int32), axis=0).astype(jnp.float32)
        pixels = members.astype(jnp.float32)
        scores = jnp.einsum("kbf,if->ikb", fetched, pixels, precision=lax.Precision.HIGHEST)
        scores = scores * scaling[:, None, None]
        live_mask = live_entry[None, :, None]
        scores = jnp.where(live_mask, scores, jnp.float32(-1e30))
        row_peak = jnp.max(scores, axis=(1, 2), keepdims=True)
        exponent = jnp.where(live_mask, jnp.exp(scores - row_peak), jnp.float32(0.0))
        row_total = jnp.sum(exponent, axis=(1, 2), keepdims=True)
        weights = (exponent / row_total).astype(jnp.bfloat16)
        block_sums = jnp.einsum("ikb,if->kbf", weights.astype(jnp.float32), pixels, precision=lax.Precision.HIGHEST)
        block_sums = block_sums.astype(jnp.bfloat16)
        running_total = running_total.at[chosen.astype(jnp.int32)].add(block_sums.astype(jnp.float32))
        return running_total, (row_peak + jnp.log(row_total)).reshape(-1)

    initial_partial_sums = jnp.zeros((NBLK, BLOCK, F), jnp.float32)
    running_total, marginal_likelihood = lax.scan(visit_block, initial_partial_sums, (images_by_group, noise_scale_factors, group_search_blocks, search_list_count))
    return running_total.reshape(NPROJ, F), marginal_likelihood.reshape(-1)
```

```python
import jax
import jax.numpy as jnp
from jax import lax
from jax.sharding import PartitionSpec as P

BLOCK = 128
CAP = 2
MAXL = 16


def on_device(images, inverse_noise_scale, projections, group_search_blocks, search_list_count):
    group_rows, pixels = images.shape
    n_groups = lax.axis_size("img")
    n_shares = lax.axis_size("pix")
    share_rows = group_rows // n_shares
    owned_blocks = projections.shape[0] // BLOCK
    own_index = lax.axis_index("img")
    first_row = lax.axis_index("pix") * share_rows
    everyone = lax.all_gather(images, "img", axis=0, tiled=True).reshape(
        n_groups, group_rows, pixels
    )
    small = jnp.concatenate(
        [group_search_blocks.astype(jnp.float32), search_list_count[:, None].astype(jnp.float32),
         lax.dynamic_slice_in_dim(inverse_noise_scale, first_row, share_rows)[None]], axis=1)
    table = lax.all_gather(small, "img", axis=0, tiled=True)
    every_list = table[:, :MAXL].astype(jnp.int32)
    every_count = table[:, MAXL].astype(jnp.int32)
    scaling = table[:, MAXL + 1:]
    positions = jnp.arange(MAXL, dtype=jnp.int32)
    slot_ids = jnp.arange(CAP, dtype=jnp.int32)
    live_entry = positions[None, :] < every_count[:, None]
    local_hit = live_entry & (every_list // owned_blocks == own_index)
    slot_rank = jnp.cumsum(local_hit.astype(jnp.int32), axis=1) - 1
    slot_pick = local_hit[:, None, :] & (slot_rank[:, None, :] == slot_ids[None, :, None])
    slot_offset = jnp.sum(jnp.where(slot_pick, every_list[:, None, :] % owned_blocks, 0), axis=2)
    slot_filled = jnp.any(slot_pick, axis=2)
    stacked = projections.reshape(owned_blocks, BLOCK, pixels)
    outgoing = jnp.take(stacked, slot_offset.reshape(-1), axis=0).reshape(
        n_groups, CAP * BLOCK, pixels
    )
    local_scores = jnp.einsum(
        "gif,gsf->gis", everyone, outgoing, preferred_element_type=jnp.float32
    )
    scores = lax.psum_scatter(local_scores, "pix", scatter_dimension=1, tiled=True)
    live = jnp.repeat(slot_filled, BLOCK, axis=1)[:, None, :]
    logits = jnp.where(live, scores * scaling[:, :, None], jnp.float32(-1e30))
    peak = jnp.max(logits, axis=2)
    total = jnp.sum(jnp.where(live, jnp.exp(logits - peak[:, :, None]), 0.0), axis=2)
    stats = lax.all_gather(jnp.stack([peak, total]), "img", axis=0)
    row_peak = jnp.max(stats[:, 0], axis=0)
    row_total = jnp.sum(stats[:, 1] * jnp.exp(stats[:, 0] - row_peak[None]), axis=0)
    evidence = row_peak + jnp.log(row_total)
    evidence_out = lax.dynamic_index_in_dim(evidence, own_index, 0, keepdims=False)
    exponent = jnp.where(live, jnp.exp(logits - row_peak[:, :, None]), 0.0)
    weights = (exponent / row_total[:, :, None]).astype(jnp.bfloat16)
    weights = lax.all_gather(weights, "pix", axis=1, tiled=True)
    arriving = jnp.einsum(
        "gis,gif->gsf", weights, everyone, preferred_element_type=jnp.float32
    ).astype(jnp.bfloat16)
    placement = (
        slot_offset.reshape(-1)[None, :] == jnp.arange(owned_blocks, dtype=jnp.int32)[:, None]
    ) & slot_filled.reshape(-1)[None, :]
    running_total = jnp.dot(
        placement.astype(jnp.bfloat16),
        arriving.reshape(n_groups * CAP, BLOCK * pixels),
        preferred_element_type=jnp.float32,
    )
    return (running_total.reshape(owned_blocks * BLOCK, pixels), evidence_out)


def solution(mesh):
    placed = (P("img", "pix"), P("img"), P("img", "pix"), P("img", None), P("img"))
    return jax.shard_map(
        on_device,
        mesh=mesh,
        in_specs=placed,
        out_specs=(P("img", "pix"), P(("img", "pix"))),
        check_vma=False,
    )
```

```python
import functools

import jax
import jax.numpy as jnp
from jax import lax
from jax.experimental import pallas as pl
from jax.experimental.pallas import tpu as pltpu
from jax.sharding import PartitionSpec as P

BLOCK = 128
CAP = 2
MAXL = 16
SIDE = 4
GROUPS = SIDE * SIDE
XS = 4
CHUNKS = 3
ROWS = 128
HALF = ROWS // 2
QUART = HALF // 2
SLOTS = CAP * BLOCK
MESH = pl.DeviceIdType.MESH


def gather_kernel(
    images, projections, ids, scales,
    everyone_out, weights_out, table_out, evidence_out,
    gath, proj, ids_all, scales_all, table, table_s, part, pair_in, x_in, logit, stats, wts, evid,
    ag_send, ag_recv, id_send, id_recv, sc_send, sc_recv, pair_send, pair_recv, x_send, x_recv,
    st_send, st_recv, w_send, w_recv, ev_send, ev_recv, local_sem,
):
    me = lax.axis_index("img")
    pix = lax.axis_index("pix")
    y, z = me // SIDE, lax.rem(me, SIDE)
    x, core = pix // 2, lax.rem(pix, 2)
    partner = 2 * x + 1 - core
    drains = []

    def remote(src, dst, ssem, rsem, device):
        return pltpu.make_async_remote_copy(
            src_ref=src, dst_ref=dst, send_sem=ssem, recv_sem=rsem,
            device_id=device, device_id_type=MESH,
        )

    def send(src, dst, ssem, rsem, device):
        copy = remote(src, dst, ssem, rsem, device)
        copy.start()
        drains.append(copy)

    def arrived(ref, ssem, rsem, device):
        remote(ref, ref, ssem, rsem, device).wait_recv()

    img_peers = [lax.rem(me + k, GROUPS) for k in range(1, GROUPS)]
    pix_peers = [lax.rem(pix + k, 2 * XS) for k in range(1, 2 * XS)]

    loads = []
    for c in range(CHUNKS):
        rows = pl.ds(c * ROWS, ROWS)
        load = pltpu.make_async_copy(images.at[rows, :], gath.at[me, rows, :], local_sem.at[c])
        load.start()
        loads.append(load)
    proj_load = pltpu.make_async_copy(projections, proj, local_sem.at[CHUNKS])
    proj_load.start()
    ids_load = pltpu.make_async_copy(ids, ids_all.at[me], local_sem.at[CHUNKS + 1])
    ids_load.start()
    scales_load = pltpu.make_async_copy(scales, scales_all.at[me], local_sem.at[CHUNKS + 2])
    scales_load.start()

    barrier = pltpu.get_barrier_semaphore()
    for peer in img_peers:
        pl.semaphore_signal(barrier, inc=1, device_id={"img": peer}, device_id_type=MESH)
    for peer in pix_peers:
        pl.semaphore_signal(barrier, inc=1, device_id={"pix": peer}, device_id_type=MESH)
    pl.semaphore_wait(barrier, len(img_peers) + len(pix_peers))

    def group(h, a, b):
        a, b = lax.rem(a + 2 * SIDE, SIDE), lax.rem(b + 2 * SIDE, SIDE)
        return a * SIDE + b if h == 0 else b * SIDE + a

    own = [(y, z), (z, y)]

    def slot(g, c, h, part_of=None):
        first, size = c * ROWS + h * HALF, HALF
        if part_of is not None:
            first, size = first + part_of * QUART, QUART
        return gath.at[g, pl.ds(first, size), :]

    def sems(c, h, k):
        at = (c * 2 + h) * 20 + k
        return ag_send.at[at], ag_recv.at[at]

    STEP = (1, -1)
    ORDER = (0, -1, 1, 2)

    def p1_own(c):
        loads[c].wait()
        for h in range(2):
            a, b = own[h]
            for k in range(2):
                ref = slot(me, c, h)
                send(ref, ref, *sems(c, h, k), {"img": group(h, a + STEP[k], b)})

    def p2_send(c, h, i):
        a, b = own[h]
        for k in range(2):
            ref = slot(group(h, a + ORDER[i], b), c, h)
            send(ref, ref, *sems(c, h, 4 + 2 * i + k), {"img": group(h, a, b + STEP[k])})

    def stage1(c):
        for h in range(2):
            p2_send(c, h, 0)
        for k in range(2):
            for h in range(2):
                a, b = own[h]
                g = group(h, a - STEP[k], b)
                arrived(slot(g, c, h), *sems(c, h, k), {"img": g})
                ref = slot(g, c, h, k)
                send(ref, ref, *sems(c, h, 2 + k), {"img": group(h, a + STEP[k], b)})
                p2_send(c, h, 1 + k)

    def stage2(c):
        for h in range(2):
            a, b = own[h]
            for k in range(2):
                arrived(
                    slot(group(h, a + 2, b), c, h, k), *sems(c, h, 2 + k),
                    {"img": group(h, a - STEP[k], b)},
                )
            p2_send(c, h, 3)

    def stage3(c):
        for i in range(4):
            for h in range(2):
                a, b = own[h]
                for k in range(2):
                    g = group(h, a + ORDER[i], b - STEP[k])
                    source = {"img": group(h, a, b - STEP[k])}
                    arrived(slot(g, c, h), *sems(c, h, 4 + 2 * i + k), source)
                    ref = slot(g, c, h, k)
                    send(ref, ref, *sems(c, h, 12 + 2 * i + k), {"img": group(h, a, b + STEP[k])})

    def stage4(c):
        for i in range(4):
            for h in range(2):
                a, b = own[h]
                for k in range(2):
                    arrived(
                        slot(group(h, a + ORDER[i], b + 2), c, h, k), *sems(c, h, 12 + 2 * i + k),
                        {"img": group(h, a, b - STEP[k])},
                    )

    def exchange_lists():
        ids_load.wait()
        scales_load.wait()
        for k, peer in enumerate(img_peers):
            send(ids_all.at[me], ids_all.at[me], id_send.at[k], id_recv.at[k], {"img": peer})
            send(scales_all.at[me], scales_all.at[me], sc_send.at[k], sc_recv.at[k], {"img": peer})

    def build_table():
        for k in range(GROUPS - 1):
            source = lax.rem(me + GROUPS - 1 - k, GROUPS)
            arrived(ids_all.at[source], id_send.at[k], id_recv.at[k], {"img": source})
            arrived(scales_all.at[source], sc_send.at[k], sc_recv.at[k], {"img": source})
        lists = ids_all[:, 0, :]
        counts = ids_all[:, 1, :]
        lane = lax.broadcasted_iota(jnp.int32, (GROUPS, 128), 1)
        hit = (lane < counts) & ((lists >> 3) == me) & (lane < MAXL)
        first = jnp.min(jnp.where(hit, lane, 128), axis=1, keepdims=True)
        last = jnp.max(jnp.where(hit, lane, -1), axis=1, keepdims=True)
        two = last > first
        offset = lists & 7
        off0 = jnp.sum(jnp.where(lane == first, offset, 0), axis=1, keepdims=True)
        off1 = jnp.sum(jnp.where((lane == last) & two, offset, 0), axis=1, keepdims=True)
        whole = (GROUPS, 128)
        table[0] = jnp.broadcast_to(off0, whole)
        table[1] = jnp.broadcast_to(off1, whole)
        table[2] = jnp.broadcast_to((first < 128).astype(jnp.int32), whole)
        table[3] = jnp.broadcast_to(two.astype(jnp.int32), whole)
        to_smem = pltpu.make_async_copy(table, table_s, local_sem.at[CHUNKS + 3])
        to_smem.start()
        to_smem.wait()
        proj_load.wait()

    def score(c, g):
        rows = gath[g, pl.ds(c * ROWS, ROWS), :]
        for s in range(CAP):
            value = lax.dot_general(
                proj[table_s[s, g, 0]], rows, (((1,), (1,)), ((), ())),
                preferred_element_type=jnp.float32,
            )
            first = pl.multiple_of(lax.rem(g, 2) * SLOTS + s * BLOCK, BLOCK)
            part[c, g // 2, pl.ds(first, BLOCK), :] = value

    def near(v):
        return v + v // 2

    def scores_early(c):
        @pl.loop(0, 9)
        def _(k):
            score(c, group(0, y + near(k // 3), z + near(lax.rem(k, 3))))

    def scores_late(c):
        @pl.loop(0, 4)
        def _(k):
            score(c, group(0, y + 2, z + k))

        @pl.loop(0, 3)
        def _(k):
            score(c, group(0, y + near(k), z + 2))

        for t in range(XS):
            send(part.at[c, 2 * t + 1 - core], pair_in.at[c, t],
                 pair_send.at[c * XS + t], pair_recv.at[c * XS + t], {"pix": partner})

    def post_pair(c):
        for d in (1, 2, 3, 0):
            t = lax.rem(x + d, XS)
            arrived_pair(c, d)
            mine = 2 * t + core
            part[c, mine] = part[c, mine] + pair_in[c, t]
            if d:
                at = c * 3 + d - 1
                send(part.at[c, mine], x_in.at[c, d - 1], x_send.at[at], x_recv.at[at],
                     {"pix": mine})

    def arrived_pair(c, d):
        if d == 1:
            for t in range(XS):
                at = c * XS + t
                arrived(pair_in.at[c, t], pair_send.at[at], pair_recv.at[at], {"pix": partner})

    def filled(g):
        return (table[2, pl.ds(g, 1), :] > 0, table[3, pl.ds(g, 1), :] > 0)

    def post_stats(c):
        for d in (1, 2, 3):
            at = c * 3 + d - 1
            arrived(x_in.at[c, d - 1], x_send.at[at], x_recv.at[at],
                    {"pix": 2 * lax.rem(x + XS - d, XS) + core})
        for j in range(2):
            g = 2 * pix + j
            scaling = scales_all[g, c:c + 1, :]
            live = filled(g)
            peak = jnp.full((1, ROWS), -1e30, jnp.float32)
            for s in range(CAP):
                at = pl.ds(j * SLOTS + s * BLOCK, BLOCK)
                total = (part[c, pix, at, :] + x_in[c, 0, at, :]) + (x_in[c, 1, at, :] + x_in[c, 2, at, :])
                value = jnp.where(live[s], total * scaling, jnp.float32(-1e30))
                logit[at, :] = value
                peak = jnp.maximum(peak, jnp.max(value, axis=0, keepdims=True))
            run = jnp.zeros((1, ROWS), jnp.float32)
            for s in range(CAP):
                value = logit[pl.ds(j * SLOTS + s * BLOCK, BLOCK), :]
                value = jnp.where(live[s], jnp.exp(value - peak), 0.0)
                run = run + jnp.sum(value, axis=0, keepdims=True)
            stats[c, me, j:j + 1, :] = peak
            stats[c, me, 2 + j:3 + j, :] = run
        for k, peer in enumerate(img_peers):
            at = c * (GROUPS - 1) + k
            send(stats.at[c, me], stats.at[c, me], st_send.at[at], st_recv.at[at], {"img": peer})

    def weight_slot(c, p):
        return wts.at[pl.ds(2 * p, 2), :, pl.ds(c * ROWS, ROWS)]

    def post_weights(c):
        for k in range(GROUPS - 1):
            at = c * (GROUPS - 1) + k
            source = lax.rem(me + GROUPS - 1 - k, GROUPS)
            arrived(stats.at[c, source], st_send.at[at], st_recv.at[at], {"img": source})
        for j in range(2):
            g = 2 * pix + j
            live = filled(g)
            peaks = stats[c, :, j, :]
            peak = jnp.max(peaks, axis=0, keepdims=True)
            total = jnp.sum(stats[c, :, 2 + j, :] * jnp.exp(peaks - peak), axis=0, keepdims=True)
            evid[pix, j * CHUNKS + c:j * CHUNKS + c + 1, :] = peak + jnp.log(total)
            inverse = 1.0 / total
            for s in range(CAP):
                value = logit[pl.ds(j * SLOTS + s * BLOCK, BLOCK), :]
                value = jnp.where(live[s], jnp.exp(value - peak) * inverse, 0.0)
                wts[g, pl.ds(s * BLOCK, BLOCK), pl.ds(c * ROWS, ROWS)] = value.astype(jnp.bfloat16)
        mine = weight_slot(c, pix)
        for d in (1, 2, 3):
            at = c * 7 + d
            send(mine, mine, w_send.at[at], w_recv.at[at],
                 {"pix": 2 * lax.rem(x + d, XS) + core})
        send(mine, mine, w_send.at[c * 7], w_recv.at[c * 7], {"pix": partner})

    def post_relay(c):
        for d in (1, 3, 2):
            source = 2 * lax.rem(x + XS - d, XS) + core
            ref = weight_slot(c, source)
            arrived(ref, w_send.at[c * 7 + d], w_recv.at[c * 7 + d], {"pix": source})
            send(ref, ref, w_send.at[c * 7 + 3 + d], w_recv.at[c * 7 + 3 + d], {"pix": partner})

    def post_weights_in(c):
        arrived(weight_slot(c, partner), w_send.at[c * 7], w_recv.at[c * 7], {"pix": partner})
        for d in (1, 3, 2):
            ref = weight_slot(c, 2 * lax.rem(x + XS - d, XS) + 1 - core)
            arrived(ref, w_send.at[c * 7 + 3 + d], w_recv.at[c * 7 + 3 + d], {"pix": partner})

    stores = []

    def store_images(c):
        rows = pl.ds(c * ROWS, ROWS)
        store = pltpu.make_async_copy(
            gath.at[:, rows, :], everyone_out.at[:, rows, :], local_sem.at[CHUNKS + 4 + c]
        )
        store.start()
        stores.append(store)

    p1_own(0)
    exchange_lists()
    stage1(0)
    build_table()
    for c in range(CHUNKS):
        stage2(c)
        if c + 1 < CHUNKS:
            p1_own(c + 1)
        if c:
            post_pair(c - 1)
        stage3(c)
        if c + 1 < CHUNKS:
            stage1(c + 1)
        if c:
            post_stats(c - 1)
        scores_early(c)
        if c:
            post_weights(c - 1)
        stage4(c)
        if c:
            post_relay(c - 1)
        scores_late(c)
        store_images(c)
    last = CHUNKS - 1
    post_pair(last)
    post_stats(last)
    post_weights(last)
    for k, peer in enumerate(pix_peers):
        send(evid.at[pix], evid.at[pix], ev_send.at[k], ev_recv.at[k], {"pix": peer})
    post_relay(last)
    for c in range(CHUNKS):
        post_weights_in(c)
    save_w = pltpu.make_async_copy(wts, weights_out, local_sem.at[2 * CHUNKS + 4])
    save_w.start()
    for k in range(2 * XS - 1):
        source = lax.rem(pix + 2 * XS - 1 - k, 2 * XS)
        arrived(evid.at[source], ev_send.at[k], ev_recv.at[k], {"pix": source})
    evidence_out[...] = evid[me // 2]
    table_out[...] = table[...]
    for copy in drains:
        copy.wait_send()
    for store in stores:
        store.wait()
    save_w.wait()


def gather_and_weigh(images, projections, ids, scales):
    rows, pixels = images.shape
    dma = pltpu.SemaphoreType.DMA
    any_space = pl.BlockSpec(memory_space=pl.ANY)
    vmem = pl.BlockSpec(memory_space=pltpu.VMEM)
    n_img, n_pix = GROUPS - 1, 2 * XS - 1
    return pl.pallas_call(
        gather_kernel,
        out_shape=(
            jax.ShapeDtypeStruct((GROUPS, rows, pixels), jnp.bfloat16),
            jax.ShapeDtypeStruct((GROUPS, SLOTS, rows), jnp.bfloat16),
            jax.ShapeDtypeStruct((4, GROUPS, 128), jnp.int32),
            jax.ShapeDtypeStruct((8, 128), jnp.float32),
        ),
        in_specs=[any_space] * 4,
        out_specs=(any_space, any_space, vmem, vmem),
        scratch_shapes=[
            pltpu.VMEM((GROUPS, rows, pixels), jnp.bfloat16),
            pltpu.VMEM(projections.shape, jnp.bfloat16),
            pltpu.VMEM((GROUPS, 8, 128), jnp.int32),
            pltpu.VMEM((GROUPS, 8, 128), jnp.float32),
            pltpu.VMEM((4, GROUPS, 128), jnp.int32),
            pltpu.SMEM((4, GROUPS, 128), jnp.int32),
            pltpu.VMEM((CHUNKS, 2 * XS, 2 * SLOTS, ROWS), jnp.float32),
            pltpu.VMEM((CHUNKS, XS, 2 * SLOTS, ROWS), jnp.float32),
            pltpu.VMEM((CHUNKS, 3, 2 * SLOTS, ROWS), jnp.float32),
            pltpu.VMEM((2 * SLOTS, ROWS), jnp.float32),
            pltpu.VMEM((CHUNKS, GROUPS, 8, ROWS), jnp.float32),
            pltpu.VMEM((GROUPS, SLOTS, rows), jnp.bfloat16),
            pltpu.VMEM((2 * XS, 8, 128), jnp.float32),
            dma((CHUNKS * 40,)), dma((CHUNKS * 40,)),
            dma((n_img,)), dma((n_img,)),
            dma((n_img,)), dma((n_img,)),
            dma((CHUNKS * XS,)), dma((CHUNKS * XS,)),
            dma((CHUNKS * 3,)), dma((CHUNKS * 3,)),
            dma((CHUNKS * n_img,)), dma((CHUNKS * n_img,)),
            dma((CHUNKS * 7,)), dma((CHUNKS * 7,)),
            dma((n_pix,)), dma((n_pix,)),
            dma((2 * CHUNKS + 5,)),
        ],
        compiler_params=pltpu.CompilerParams(
            collective_id=0, has_side_effects=True, vmem_limit_bytes=60 * 1024 * 1024
        ),
        name="gather_and_weigh",
    )(images, projections, ids, scales)


def sum_kernel(table, images, weights, out):
    g = pl.program_id(1)

    @pl.when(g == 0)
    def _():
        out[...] = jnp.zeros_like(out)

    value = jnp.dot(weights[0], images[0], preferred_element_type=jnp.float32)
    for s in range(CAP):
        at = pl.multiple_of(table[s, g, 0] * BLOCK, BLOCK)
        out[pl.ds(at, BLOCK), :] += value[s * BLOCK:(s + 1) * BLOCK]


def sum_images(table, images, weights, owned):
    groups, rows, pixels = images.shape
    tile = pixels // 2
    return pl.pallas_call(
        sum_kernel,
        out_shape=jax.ShapeDtypeStruct((owned, pixels), jnp.float32),
        grid_spec=pltpu.PrefetchScalarGridSpec(
            num_scalar_prefetch=1,
            grid=(pixels // tile, groups),
            in_specs=[
                pl.BlockSpec((1, rows, tile), lambda f, g, table: (g, 0, f)),
                pl.BlockSpec((1, SLOTS, rows), lambda f, g, table: (g, 0, 0)),
            ],
            out_specs=pl.BlockSpec((owned, tile), lambda f, g, table: (0, f)),
        ),
        compiler_params=pltpu.CompilerParams(
            dimension_semantics=("arbitrary", "arbitrary"), vmem_limit_bytes=48 * 1024 * 1024
        ),
        name="sum_images",
    )(table, images, weights)


def on_device(images, inverse_noise_scale, projections, group_search_blocks, search_list_count):
    group_rows = images.shape[0]
    share_rows = group_rows // lax.axis_size("pix")
    ids = jnp.concatenate([
        jnp.pad(group_search_blocks, ((0, 0), (0, 128 - MAXL))),
        jnp.broadcast_to(search_list_count[:, None], (7, 128)),
    ])
    scales = jnp.pad(inverse_noise_scale.reshape(CHUNKS, ROWS), ((0, 8 - CHUNKS), (0, 0)))
    everyone, weights, table, evidence = gather_and_weigh(
        images, projections.reshape(-1, BLOCK, projections.shape[1]), ids, scales
    )
    sums = sum_images(table, everyone, weights, projections.shape[0])
    odd = lax.rem(lax.axis_index("img"), 2)
    own = lax.dynamic_slice_in_dim(evidence, odd * CHUNKS, CHUNKS, axis=0).reshape(-1)
    first_row = lax.axis_index("pix") * share_rows
    return sums, lax.dynamic_slice_in_dim(own, first_row, share_rows)


def solution(mesh):
    placed = (P("img", "pix"), P("img"), P("img", "pix"), P("img", None), P("img"))
    return jax.shard_map(
        on_device,
        mesh=mesh,
        in_specs=placed,
        out_specs=(P("img", "pix"), P(("img", "pix"))),
        check_vma=False,
    )
```

```python
import functools

import jax
import jax.numpy as jnp
from jax import lax
from jax.experimental import pallas as pl
from jax.experimental.pallas import tpu as pltpu
from jax.sharding import PartitionSpec as P

BLOCK = 128
CAP = 2
MAXL = 16
SIDE = 4
GROUPS = SIDE * SIDE
XS = 4
FIRST = (0, 128, 256, 320)
SIZE = (128, 128, 64, 64)
CHUNKS = len(SIZE)
WHOLE = 2
ROWS = 128
COLS = 512
SLOTS = CAP * BLOCK
MESH = pl.DeviceIdType.MESH


def gather_kernel(
    images, projections, ids, count, scales,
    late_images, late_weights, early_sums, pairs_out, evidence_out,
    gath, proj, ids_all, scales_all, table, table_s, part_w, part_h, pair_w, pair_h, x_w, x_h,
    logit, stats, wts_w, wts_h, wfull, acc, evid,
    ag_send, ag_recv, id_send, id_recv, sc_send, sc_recv, pair_send, pair_recv, x_send, x_recv,
    st_send, st_recv, w_send, w_recv, ev_send, ev_recv, local_sem,
):
    me = lax.axis_index("img")
    pix = lax.axis_index("pix")
    y, z = me // SIDE, lax.rem(me, SIDE)
    x, core = pix // 2, lax.rem(pix, 2)
    partner = 2 * x + 1 - core
    drains = []
    lane = lax.broadcasted_iota(jnp.int32, (1, 128), 1)
    low = lane < 64

    def remote(src, dst, ssem, rsem, device):
        return pltpu.make_async_remote_copy(
            src_ref=src, dst_ref=dst, send_sem=ssem, recv_sem=rsem,
            device_id=device, device_id_type=MESH,
        )

    def send(src, dst, ssem, rsem, device):
        copy = remote(src, dst, ssem, rsem, device)
        copy.start()
        drains.append(copy)

    def arrived(ref, ssem, rsem, device):
        remote(ref, ref, ssem, rsem, device).wait_recv()

    img_peers = [lax.rem(me + k, GROUPS) for k in range(1, GROUPS)]
    pix_peers = [lax.rem(pix + k, 2 * XS) for k in range(1, 2 * XS)]

    def part(c):
        return part_w.at[c] if c < WHOLE else part_h.at[c - WHOLE]

    def pair_in(c):
        return pair_w.at[c] if c < WHOLE else pair_h.at[c - WHOLE]

    def x_in(c):
        return x_w.at[c] if c < WHOLE else x_h.at[c - WHOLE]

    loads = []
    for c in range(CHUNKS):
        rows = pl.ds(FIRST[c], SIZE[c])
        load = pltpu.make_async_copy(images.at[rows, :], gath.at[me, rows, :], local_sem.at[c])
        load.start()
        loads.append(load)
    proj_load = pltpu.make_async_copy(projections, proj, local_sem.at[CHUNKS])
    proj_load.start()
    ids_all[me, 0:1, 0:MAXL] = ids[...]
    ids_all[me, 1:2, :] = jnp.full((1, 128), count[0], jnp.int32)
    scales_all[me, 0:3, :] = scales[...]

    barrier = pltpu.get_barrier_semaphore()
    for peer in img_peers:
        pl.semaphore_signal(barrier, inc=1, device_id={"img": peer}, device_id_type=MESH)
    for peer in pix_peers:
        pl.semaphore_signal(barrier, inc=1, device_id={"pix": peer}, device_id_type=MESH)
    pl.semaphore_wait(barrier, len(img_peers) + len(pix_peers))

    def group(h, a, b):
        a, b = lax.rem(a + 2 * SIDE, SIDE), lax.rem(b + 2 * SIDE, SIDE)
        return a * SIDE + b if h == 0 else b * SIDE + a

    own = [(y, z), (z, y)]

    def slot(g, c, h, part_of=None):
        size = SIZE[c] // 2
        first = FIRST[c] + h * size
        if part_of is not None:
            size //= 2
            first += part_of * size
        return gath.at[g, pl.ds(first, size), :]

    def sems(c, h, k):
        at = (c * 2 + h) * 20 + k
        return ag_send.at[at], ag_recv.at[at]

    STEP = (1, -1)
    ORDER = (0, -1, 1, 2)

    def p1_own(c):
        loads[c].wait()
        for h in range(2):
            a, b = own[h]
            for k in range(2):
                ref = slot(me, c, h)
                send(ref, ref, *sems(c, h, k), {"img": group(h, a + STEP[k], b)})

    def p2_send(c, h, i):
        a, b = own[h]
        for k in range(2):
            ref = slot(group(h, a + ORDER[i], b), c, h)
            send(ref, ref, *sems(c, h, 4 + 2 * i + k), {"img": group(h, a, b + STEP[k])})

    def stage1(c):
        for h in range(2):
            p2_send(c, h, 0)
        for k in range(2):
            for h in range(2):
                a, b = own[h]
                g = group(h, a - STEP[k], b)
                arrived(slot(g, c, h), *sems(c, h, k), {"img": g})
                ref = slot(g, c, h, k)
                send(ref, ref, *sems(c, h, 2 + k), {"img": group(h, a + STEP[k], b)})
                p2_send(c, h, 1 + k)

    def stage2(c):
        for h in range(2):
            a, b = own[h]
            for k in range(2):
                arrived(
                    slot(group(h, a + 2, b), c, h, k), *sems(c, h, 2 + k),
                    {"img": group(h, a - STEP[k], b)},
                )
            p2_send(c, h, 3)

    def stage3(c, shards):
        for i in shards:
            for h in range(2):
                a, b = own[h]
                for k in range(2):
                    g = group(h, a + ORDER[i], b - STEP[k])
                    source = {"img": group(h, a, b - STEP[k])}
                    arrived(slot(g, c, h), *sems(c, h, 4 + 2 * i + k), source)
                    ref = slot(g, c, h, k)
                    send(ref, ref, *sems(c, h, 12 + 2 * i + k), {"img": group(h, a, b + STEP[k])})

    def stage4(c):
        for i in range(4):
            for h in range(2):
                a, b = own[h]
                for k in range(2):
                    arrived(
                        slot(group(h, a + ORDER[i], b + 2), c, h, k), *sems(c, h, 12 + 2 * i + k),
                        {"img": group(h, a, b - STEP[k])},
                    )

    def exchange_lists():
        for k, peer in enumerate(img_peers):
            send(ids_all.at[me], ids_all.at[me], id_send.at[k], id_recv.at[k], {"img": peer})
            send(scales_all.at[me], scales_all.at[me], sc_send.at[k], sc_recv.at[k], {"img": peer})

    def build_table():
        for k in range(GROUPS - 1):
            source = lax.rem(me + GROUPS - 1 - k, GROUPS)
            arrived(ids_all.at[source], id_send.at[k], id_recv.at[k], {"img": source})
            arrived(scales_all.at[source], sc_send.at[k], sc_recv.at[k], {"img": source})
        lists = ids_all[:, 0, :]
        counts = ids_all[:, 1, :]
        at = lax.broadcasted_iota(jnp.int32, (GROUPS, 128), 1)
        hit = (at < counts) & ((lists >> 3) == me) & (at < MAXL)
        first = jnp.min(jnp.where(hit, at, 128), axis=1, keepdims=True)
        last = jnp.max(jnp.where(hit, at, -1), axis=1, keepdims=True)
        two = last > first
        offset = lists & 7
        off0 = jnp.sum(jnp.where(at == first, offset, 0), axis=1, keepdims=True)
        off1 = jnp.sum(jnp.where((at == last) & two, offset, 0), axis=1, keepdims=True)
        whole = (GROUPS, 128)
        table[0] = jnp.broadcast_to(off0, whole)
        table[1] = jnp.broadcast_to(off1, whole)
        table[2] = jnp.broadcast_to((first < 128).astype(jnp.int32), whole)
        table[3] = jnp.broadcast_to(two.astype(jnp.int32), whole)
        to_smem = pltpu.make_async_copy(table, table_s, local_sem.at[CHUNKS + 1])
        to_smem.start()
        for s in range(CAP):
            for p in range(GROUPS // 2):
                pairs_out[s, p:p + 1, :] = jnp.where(
                    low, table[s, 2 * p:2 * p + 1, :], table[s, 2 * p + 1:2 * p + 2, :])
        to_smem.wait()
        proj_load.wait()

    def against(block, rows):
        return lax.dot_general(
            proj[block], rows, (((1,), (1,)), ((), ())), preferred_element_type=jnp.float32)

    def score(c, g):
        rows = gath[g, pl.ds(FIRST[c], ROWS), :]
        for s in range(CAP):
            first = pl.multiple_of(lax.rem(g, 2) * SLOTS + s * BLOCK, BLOCK)
            part_w[c, g // 2, pl.ds(first, BLOCK), :] = against(table_s[s, g, 0], rows)

    def score_pair(c, t):
        rows = gath[pl.ds(2 * t, 2), pl.ds(FIRST[c], 64), :].reshape(ROWS, gath.shape[2])
        for s in range(CAP):
            one = against(table_s[s, 2 * t, 0], rows)
            other = against(table_s[s, 2 * t + 1, 0], rows)
            part_h[c - WHOLE, t, s * BLOCK:(s + 1) * BLOCK, :] = jnp.where(low, one, other)

    def near(v):
        return v + v // 2

    def row_of(v):
        return lax.rem(y + v, SIDE)

    def scores_early(c):
        if c < WHOLE:
            @pl.loop(0, 9)
            def _(k):
                score(c, group(0, y + near(k // 3), z + near(lax.rem(k, 3))))
        else:
            @pl.loop(0, 3)
            def _(k):
                score_pair(c, 2 * row_of(near(k)) + z // 2)

    def scores_late(c):
        if c < WHOLE:
            @pl.loop(0, 4)
            def _(k):
                score(c, group(0, y + 2, z + k))

            @pl.loop(0, 3)
            def _(k):
                score(c, group(0, y + near(k), z + 2))
        else:
            @pl.loop(0, 3)
            def _(k):
                score_pair(c, 2 * row_of(near(k)) + 1 - z // 2)

            @pl.loop(0, 2)
            def _(k):
                score_pair(c, 2 * row_of(2) + k)

        for t in range(XS):
            send(part(c).at[2 * t + 1 - core], pair_in(c).at[t],
                 pair_send.at[c * XS + t], pair_recv.at[c * XS + t], {"pix": partner})

    def post_pair(c):
        for t in range(XS):
            at = c * XS + t
            arrived(pair_in(c).at[t], pair_send.at[at], pair_recv.at[at], {"pix": partner})
        for d in (2, 1, 3, 0):
            t = lax.rem(x + d, XS)
            mine = 2 * t + core
            part(c)[mine] = part(c)[mine] + pair_in(c)[t]
            if d:
                at = c * 3 + d - 1
                send(part(c).at[mine], x_in(c).at[d - 1], x_send.at[at], x_recv.at[at],
                     {"pix": mine})

    def units(c):
        return range(2 if c < WHOLE else 1)

    def filled(c, j):
        rows = []
        for s in range(CAP):
            one = table[2 + s, pl.ds(2 * pix + j, 1), :]
            if c >= WHOLE:
                one = jnp.where(low, one, table[2 + s, pl.ds(2 * pix + 1, 1), :])
            rows.append(one > 0)
        return rows

    def scaling_of(c, j):
        if c < WHOLE:
            return scales_all[2 * pix + j, c:c + 1, :]
        one = scales_all[2 * pix, 2:3, :]
        other = scales_all[2 * pix + 1, 2:3, :]
        if c == WHOLE:
            return jnp.where(low, one, pltpu.roll(other, 64, 1))
        return jnp.where(low, pltpu.roll(one, 64, 1), other)

    def post_stats(c):
        for d in (1, 2, 3):
            at = c * 3 + d - 1
            arrived(x_in(c).at[d - 1], x_send.at[at], x_recv.at[at],
                    {"pix": 2 * lax.rem(x + XS - d, XS) + core})
        for j in units(c):
            scaling = scaling_of(c, j)
            live = filled(c, j)
            peak = jnp.full((1, ROWS), -1e30, jnp.float32)
            for s in range(CAP):
                at = pl.ds(j * SLOTS + s * BLOCK, BLOCK)
                others = x_in(c)
                total = (part(c)[pix, at, :] + others[0, at, :]) + (others[1, at, :] + others[2, at, :])
                value = jnp.where(live[s], total * scaling, jnp.float32(-1e30))
                logit[c, at, :] = value
                peak = jnp.maximum(peak, jnp.max(value, axis=0, keepdims=True))
            run = jnp.zeros((1, ROWS), jnp.float32)
            for s in range(CAP):
                value = logit[c, pl.ds(j * SLOTS + s * BLOCK, BLOCK), :]
                value = jnp.where(live[s], jnp.exp(value - peak), 0.0)
                run = run + jnp.sum(value, axis=0, keepdims=True)
            stats[c, me, j:j + 1, :] = peak
            stats[c, me, 2 + j:3 + j, :] = run
        for k, peer in enumerate(img_peers):
            at = c * (GROUPS - 1) + k
            send(stats.at[c, me], stats.at[c, me], st_send.at[at], st_recv.at[at], {"img": peer})

    def weight_slot(c, p):
        return wts_w.at[c, pl.ds(2 * p, 2)] if c < WHOLE else wts_h.at[c - WHOLE, p]

    def post_weights(c):
        for k in range(GROUPS - 1):
            at = c * (GROUPS - 1) + k
            source = lax.rem(me + GROUPS - 1 - k, GROUPS)
            arrived(stats.at[c, source], st_send.at[at], st_recv.at[at], {"img": source})
        for j in units(c):
            live = filled(c, j)
            peaks = stats[c, :, j, :]
            peak = jnp.max(peaks, axis=0, keepdims=True)
            total = jnp.sum(stats[c, :, 2 + j, :] * jnp.exp(peaks - peak), axis=0, keepdims=True)
            row = 2 * j + c if c < WHOLE else 2 + c
            evid[pix, row:row + 1, :] = peak + jnp.log(total)
            inverse = 1.0 / total
            for s in range(CAP):
                value = logit[c, pl.ds(j * SLOTS + s * BLOCK, BLOCK), :]
                value = jnp.where(live[s], jnp.exp(value - peak) * inverse, 0.0).astype(jnp.bfloat16)
                if c < WHOLE:
                    wts_w[c, 2 * pix + j, s * BLOCK:(s + 1) * BLOCK, :] = value
                else:
                    wts_h[c - WHOLE, pix, s * BLOCK:(s + 1) * BLOCK, :] = value
        mine = weight_slot(c, pix)
        for d in (2, 1, 3):
            at = c * 7 + d
            send(mine, mine, w_send.at[at], w_recv.at[at],
                 {"pix": 2 * lax.rem(x + d, XS) + core})
        send(mine, mine, w_send.at[c * 7], w_recv.at[c * 7], {"pix": partner})

    def post_relay(c):
        for d in (1, 3, 2):
            source = 2 * lax.rem(x + XS - d, XS) + core
            ref = weight_slot(c, source)
            arrived(ref, w_send.at[c * 7 + d], w_recv.at[c * 7 + d], {"pix": source})
            send(ref, ref, w_send.at[c * 7 + 3 + d], w_recv.at[c * 7 + 3 + d], {"pix": partner})

    def post_weights_in(c):
        arrived(weight_slot(c, partner), w_send.at[c * 7], w_recv.at[c * 7], {"pix": partner})
        for d in (1, 3, 2):
            ref = weight_slot(c, 2 * lax.rem(x + XS - d, XS) + 1 - core)
            arrived(ref, w_send.at[c * 7 + 3 + d], w_recv.at[c * 7 + 3 + d], {"pix": partner})

    def place(c):
        @pl.loop(0, GROUPS)
        def _(g):
            columns = pl.ds(pl.multiple_of(g * ROWS, ROWS), ROWS)
            for b in range(proj.shape[0]):
                value = jnp.zeros((BLOCK, ROWS), jnp.bfloat16)
                for s in range(CAP):
                    value = value + jnp.where(
                        table_s[s, g, 0] == b, wts_w[c, g, s * BLOCK:(s + 1) * BLOCK, :], jnp.bfloat16(0))
                wfull[b * BLOCK:(b + 1) * BLOCK, columns] = value

    def add_images(c, lo, hi):
        @pl.loop(lo, hi)
        def _(u):
            rows = pl.ds(pl.multiple_of(lax.rem(u, 4) * SLOTS, SLOTS), SLOTS)
            columns = pl.ds(pl.multiple_of((u // 4) * COLS, COLS), COLS)
            there = gath[:, pl.ds(FIRST[c], ROWS), columns].reshape(GROUPS * ROWS, COLS)
            value = jnp.dot(wfull[rows, :], there, preferred_element_type=jnp.float32)
            acc[rows, columns] = value if c == 0 else acc[rows, columns] + value

    stores = []

    def store(src, dst):
        copy = pltpu.make_async_copy(src, dst, local_sem.at[CHUNKS + 2 + len(stores)])
        copy.start()
        stores.append(copy)

    def store_images(c):
        store(gath.at[:, pl.ds(FIRST[c], 64), :],
              late_images.at[:, pl.ds(FIRST[c] - FIRST[WHOLE], 64), :])

    p1_own(0)
    exchange_lists()
    stage1(0)
    build_table()

    stage2(0)
    p1_own(1)
    stage3(0, range(4))
    stage1(1)
    scores_early(0)
    stage4(0)
    scores_late(0)

    stage2(1)
    p1_own(2)
    post_pair(0)
    stage3(1, (0, 1))
    post_stats(0)
    stage3(1, (2, 3))
    stage1(2)
    scores_early(1)
    post_weights(0)
    stage4(1)
    scores_late(1)

    stage2(2)
    p1_own(3)
    post_pair(1)
    stage3(2, (0, 1))
    post_relay(0)
    stage3(2, (2, 3))
    post_stats(1)
    stage1(3)
    scores_early(2)
    post_weights_in(0)
    place(0)
    add_images(0, 0, 6)
    stage4(2)
    scores_late(2)
    store_images(2)

    stage2(3)
    post_pair(2)
    post_weights(1)
    stage3(3, range(4))
    post_stats(2)
    add_images(0, 6, 16)
    scores_early(3)
    post_weights(2)
    stage4(3)
    scores_late(3)
    store_images(3)

    post_pair(3)
    post_relay(1)
    post_relay(2)
    post_weights_in(1)
    place(1)
    add_images(1, 0, 8)
    post_stats(3)
    add_images(1, 8, 16)
    store(acc, early_sums)
    post_weights(3)
    for k, peer in enumerate(pix_peers):
        send(evid.at[pix], evid.at[pix], ev_send.at[k], ev_recv.at[k], {"pix": peer})
    post_relay(3)
    post_weights_in(2)
    post_weights_in(3)
    store(wts_h, late_weights)
    for k in range(2 * XS - 1):
        source = lax.rem(pix + 2 * XS - 1 - k, 2 * XS)
        arrived(evid.at[source], ev_send.at[k], ev_recv.at[k], {"pix": source})
    odd = lax.rem(me, 2)
    mine = evid[me // 2]
    for c in range(WHOLE):
        evidence_out[c:c + 1, :] = jnp.where(odd == 0, mine[c:c + 1], mine[2 + c:3 + c])
    third, fourth = mine[4:5], mine[5:6]
    evidence_out[WHOLE:WHOLE + 1, :] = jnp.where(
        odd == 0,
        jnp.where(low, third, pltpu.roll(fourth, 64, 1)),
        jnp.where(low, pltpu.roll(third, 64, 1), fourth),
    )
    for copy in drains:
        copy.wait_send()
    for copy in stores:
        copy.wait()


def gather_and_weigh(images, projections, ids, count, scales):
    rows, pixels = images.shape
    late = rows - FIRST[WHOLE]
    owned = projections.shape[0] * BLOCK
    dma = pltpu.SemaphoreType.DMA
    any_space = pl.BlockSpec(memory_space=pl.ANY)
    vmem = pl.BlockSpec(memory_space=pltpu.VMEM)
    n_img, n_pix = GROUPS - 1, 2 * XS - 1
    f32, bf16 = jnp.float32, jnp.bfloat16
    half = CHUNKS - WHOLE
    return pl.pallas_call(
        gather_kernel,
        out_shape=(
            jax.ShapeDtypeStruct((GROUPS, late, pixels), bf16),
            jax.ShapeDtypeStruct((half, 2 * XS, SLOTS, ROWS), bf16),
            jax.ShapeDtypeStruct((owned, pixels), f32),
            jax.ShapeDtypeStruct((CAP, GROUPS // 2, ROWS), jnp.int32),
            jax.ShapeDtypeStruct((3, 128), f32),
        ),
        in_specs=[any_space, any_space, vmem, pl.BlockSpec(memory_space=pltpu.SMEM), vmem],
        out_specs=(any_space, any_space, any_space, vmem, vmem),
        scratch_shapes=[
            pltpu.VMEM((GROUPS, rows, pixels), bf16),
            pltpu.VMEM(projections.shape, bf16),
            pltpu.VMEM((GROUPS, 8, 128), jnp.int32),
            pltpu.VMEM((GROUPS, 8, 128), f32),
            pltpu.VMEM((4, GROUPS, 128), jnp.int32),
            pltpu.SMEM((4, GROUPS, 128), jnp.int32),
            pltpu.VMEM((WHOLE, 2 * XS, 2 * SLOTS, ROWS), f32),
            pltpu.VMEM((half, 2 * XS, SLOTS, ROWS), f32),
            pltpu.VMEM((WHOLE, XS, 2 * SLOTS, ROWS), f32),
            pltpu.VMEM((half, XS, SLOTS, ROWS), f32),
            pltpu.VMEM((WHOLE, 3, 2 * SLOTS, ROWS), f32),
            pltpu.VMEM((half, 3, SLOTS, ROWS), f32),
            pltpu.VMEM((CHUNKS, 2 * SLOTS, ROWS), f32),
            pltpu.VMEM((CHUNKS, GROUPS, 8, ROWS), f32),
            pltpu.VMEM((WHOLE, GROUPS, SLOTS, ROWS), bf16),
            pltpu.VMEM((half, 2 * XS, SLOTS, ROWS), bf16),
            pltpu.VMEM((owned, GROUPS * ROWS), bf16),
            pltpu.VMEM((owned, pixels), f32),
            pltpu.VMEM((2 * XS, 8, 128), f32),
            dma((CHUNKS * 40,)), dma((CHUNKS * 40,)),
            dma((n_img,)), dma((n_img,)),
            dma((n_img,)), dma((n_img,)),
            dma((CHUNKS * XS,)), dma((CHUNKS * XS,)),
            dma((CHUNKS * 3,)), dma((CHUNKS * 3,)),
            dma((CHUNKS * n_img,)), dma((CHUNKS * n_img,)),
            dma((CHUNKS * 7,)), dma((CHUNKS * 7,)),
            dma((n_pix,)), dma((n_pix,)),
            dma((CHUNKS + 6,)),
        ],
        compiler_params=pltpu.CompilerParams(
            collective_id=0, has_side_effects=True, vmem_limit_bytes=63 * 1024 * 1024
        ),
        name="gather_and_weigh",
    )(images, projections, ids, count, scales)


def sum_kernel(pairs, early, images, weights, out, wfull):
    half = weights.shape[0]
    pair_count = weights.shape[1]
    depth = pair_count * ROWS

    @pl.when(pl.program_id(0) == 0)
    def _():
        for c in range(half):
            for p in range(pair_count):
                at = [pairs[s, p:p + 1, :] for s in range(CAP)]
                value = [weights[c, p, s * BLOCK:(s + 1) * BLOCK, :].astype(jnp.float32) for s in range(CAP)]
                for b in range(wfull.shape[0] // BLOCK):
                    placed = jnp.where(at[0] == b, value[0], 0.0) + jnp.where(at[1] == b, value[1], 0.0)
                    first = (c * pair_count + p) * ROWS
                    wfull[b * BLOCK:(b + 1) * BLOCK, first:first + ROWS] = placed.astype(jnp.bfloat16)

    there = [images[:, c * 64:(c + 1) * 64, :].reshape(depth, images.shape[2]) for c in range(half)]
    for m in range(wfull.shape[0] // SLOTS):
        rows = slice(m * SLOTS, (m + 1) * SLOTS)
        value = early[rows, :]
        for c in range(half):
            value = value + jnp.dot(
                wfull[rows, c * depth:(c + 1) * depth], there[c], preferred_element_type=jnp.float32)
        out[rows, :] = value


def sum_images(pairs, early, images, weights):
    owned, pixels = early.shape
    groups, late, _ = images.shape
    tile = 512
    return pl.pallas_call(
        sum_kernel,
        out_shape=jax.ShapeDtypeStruct((owned, pixels), jnp.float32),
        grid=(pixels // tile,),
        in_specs=[
            pl.BlockSpec(pairs.shape, lambda f: (0, 0, 0)),
            pl.BlockSpec((owned, tile), lambda f: (0, f)),
            pl.BlockSpec((groups, late, tile), lambda f: (0, 0, f)),
            pl.BlockSpec(weights.shape, lambda f: (0, 0, 0, 0)),
        ],
        out_specs=pl.BlockSpec((owned, tile), lambda f: (0, f)),
        scratch_shapes=[pltpu.VMEM((owned, groups * late), jnp.bfloat16)],
        compiler_params=pltpu.CompilerParams(
            dimension_semantics=("arbitrary",), vmem_limit_bytes=48 * 1024 * 1024
        ),
        name="sum_images",
    )(pairs, early, images, weights)


def on_device(images, inverse_noise_scale, projections, group_search_blocks, search_list_count):
    group_rows, pixels = images.shape
    share_rows = group_rows // lax.axis_size("pix")
    late_images, late_weights, early, pairs, evidence = gather_and_weigh(
        images, projections.reshape(-1, BLOCK, pixels), group_search_blocks, search_list_count,
        inverse_noise_scale.reshape(-1, ROWS),
    )
    sums = sum_images(pairs, early, late_images, late_weights)
    first_row = lax.axis_index("pix") * share_rows
    return sums, lax.dynamic_slice_in_dim(evidence.reshape(-1), first_row, share_rows)


def solution(mesh):
    placed = (P("img", "pix"), P("img"), P("img", "pix"), P("img", None), P("img"))
    return jax.shard_map(
        on_device,
        mesh=mesh,
        in_specs=placed,
        out_specs=(P("img", "pix"), P(("img", "pix"))),
        check_vma=False,
    )
```

```python
import functools

import jax
import jax.numpy as jnp
from jax import lax
from jax.experimental import pallas as pl
from jax.experimental.pallas import tpu as pltpu
from jax.sharding import PartitionSpec as P

BLOCK = 128
CAP = 2
MAXL = 16
SIDE = 4
GROUPS = SIDE * SIDE
XS = 4
FIRST = (0, 128, 256, 320)
SIZE = (128, 128, 64, 64)
CHUNKS = len(SIZE)
WHOLE = 2
ROWS = 128
COLS = 512
SLOTS = CAP * BLOCK
MESH = pl.DeviceIdType.MESH


def gather_kernel(
    images, projections, ids, count, scales,
    late_images, late_weights, early_sums, pairs_out, evidence_out,
    gath, proj, ids_all, scales_all, table, table_s, part_w, part_h, pair_w, pair_h, x_w, x_h,
    logit, stats, wts_w, wts_h, wfull, acc, evid,
    ag_send, ag_recv, id_send, id_recv, sc_send, sc_recv, pair_send, pair_recv, x_send, x_recv,
    st_send, st_recv, w_send, w_recv, ev_send, ev_recv, local_sem,
):
    me = lax.axis_index("img")
    pix = lax.axis_index("pix")
    y, z = me // SIDE, lax.rem(me, SIDE)
    x, core = pix // 2, lax.rem(pix, 2)
    partner = 2 * x + 1 - core
    drains = []
    lane = lax.broadcasted_iota(jnp.int32, (1, 128), 1)
    low = lane < 64

    def remote(src, dst, ssem, rsem, device):
        return pltpu.make_async_remote_copy(
            src_ref=src, dst_ref=dst, send_sem=ssem, recv_sem=rsem,
            device_id=device, device_id_type=MESH,
        )

    def send(src, dst, ssem, rsem, device):
        copy = remote(src, dst, ssem, rsem, device)
        copy.start()
        drains.append(copy)

    def arrived(ref, ssem, rsem, device):
        remote(ref, ref, ssem, rsem, device).wait_recv()

    img_peers = [lax.rem(me + k, GROUPS) for k in range(1, GROUPS)]
    pix_peers = [lax.rem(pix + k, 2 * XS) for k in range(1, 2 * XS)]

    def part(c):
        return part_w.at[c] if c < WHOLE else part_h.at[c - WHOLE]

    def pair_in(c):
        return pair_w.at[c] if c < WHOLE else pair_h.at[c - WHOLE]

    def x_in(c):
        return x_w.at[c] if c < WHOLE else x_h.at[c - WHOLE]

    loads = []
    for c in range(CHUNKS):
        rows = pl.ds(FIRST[c], SIZE[c])
        load = pltpu.make_async_copy(images.at[rows, :], gath.at[me, rows, :], local_sem.at[c])
        load.start()
        loads.append(load)
    proj_load = pltpu.make_async_copy(projections, proj, local_sem.at[CHUNKS])
    proj_load.start()
    ids_all[me, 0:1, 0:MAXL] = ids[...]
    ids_all[me, 1:2, :] = jnp.full((1, 128), count[0], jnp.int32)
    scales_all[me, 0:3, :] = scales[...]

    barrier = pltpu.get_barrier_semaphore()
    for peer in img_peers:
        pl.semaphore_signal(barrier, inc=1, device_id={"img": peer}, device_id_type=MESH)
    for peer in pix_peers:
        pl.semaphore_signal(barrier, inc=1, device_id={"pix": peer}, device_id_type=MESH)
    pl.semaphore_wait(barrier, len(img_peers) + len(pix_peers))

    def group(h, a, b):
        a, b = lax.rem(a + 2 * SIDE, SIDE), lax.rem(b + 2 * SIDE, SIDE)
        return a * SIDE + b if h == 0 else b * SIDE + a

    own = [(y, z), (z, y)]

    def slot(g, c, h, part_of=None):
        size = SIZE[c] // 2
        first = FIRST[c] + h * size
        if part_of is not None:
            size //= 2
            first += part_of * size
        return gath.at[g, pl.ds(first, size), :]

    def sems(c, h, k):
        at = (c * 2 + h) * 20 + k
        return ag_send.at[at], ag_recv.at[at]

    STEP = (1, -1)
    ORDER = (0, -1, 1, 2)

    def p1_own(c):
        loads[c].wait()
        for h in range(2):
            a, b = own[h]
            for k in range(2):
                ref = slot(me, c, h)
                send(ref, ref, *sems(c, h, k), {"img": group(h, a + STEP[k], b)})

    def p2_send(c, h, i):
        a, b = own[h]
        for k in range(2):
            ref = slot(group(h, a + ORDER[i], b), c, h)
            send(ref, ref, *sems(c, h, 4 + 2 * i + k), {"img": group(h, a, b + STEP[k])})

    def stage1(c):
        for h in range(2):
            p2_send(c, h, 0)
        for k in range(2):
            for h in range(2):
                a, b = own[h]
                g = group(h, a - STEP[k], b)
                arrived(slot(g, c, h), *sems(c, h, k), {"img": g})
                ref = slot(g, c, h, k)
                send(ref, ref, *sems(c, h, 2 + k), {"img": group(h, a + STEP[k], b)})
                p2_send(c, h, 1 + k)

    def stage2(c):
        for h in range(2):
            a, b = own[h]
            for k in range(2):
                arrived(
                    slot(group(h, a + 2, b), c, h, k), *sems(c, h, 2 + k),
                    {"img": group(h, a - STEP[k], b)},
                )
            p2_send(c, h, 3)

    def stage3(c, shards):
        for i in shards:
            for h in range(2):
                a, b = own[h]
                for k in range(2):
                    g = group(h, a + ORDER[i], b - STEP[k])
                    source = {"img": group(h, a, b - STEP[k])}
                    arrived(slot(g, c, h), *sems(c, h, 4 + 2 * i + k), source)
                    ref = slot(g, c, h, k)
                    send(ref, ref, *sems(c, h, 12 + 2 * i + k), {"img": group(h, a, b + STEP[k])})

    def stage4(c):
        for i in range(4):
            for h in range(2):
                a, b = own[h]
                for k in range(2):
                    arrived(
                        slot(group(h, a + ORDER[i], b + 2), c, h, k), *sems(c, h, 12 + 2 * i + k),
                        {"img": group(h, a, b - STEP[k])},
                    )

    def exchange_lists():
        for k, peer in enumerate(img_peers):
            send(ids_all.at[me], ids_all.at[me], id_send.at[k], id_recv.at[k], {"img": peer})
            send(scales_all.at[me], scales_all.at[me], sc_send.at[k], sc_recv.at[k], {"img": peer})

    def build_table():
        for k in range(GROUPS - 1):
            source = lax.rem(me + GROUPS - 1 - k, GROUPS)
            arrived(ids_all.at[source], id_send.at[k], id_recv.at[k], {"img": source})
            arrived(scales_all.at[source], sc_send.at[k], sc_recv.at[k], {"img": source})
        lists = ids_all[:, 0, :]
        counts = ids_all[:, 1, :]
        at = lax.broadcasted_iota(jnp.int32, (GROUPS, 128), 1)
        hit = (at < counts) & ((lists >> 3) == me) & (at < MAXL)
        first = jnp.min(jnp.where(hit, at, 128), axis=1, keepdims=True)
        last = jnp.max(jnp.where(hit, at, -1), axis=1, keepdims=True)
        two = last > first
        offset = lists & 7
        off0 = jnp.sum(jnp.where(at == first, offset, 0), axis=1, keepdims=True)
        off1 = jnp.sum(jnp.where((at == last) & two, offset, 0), axis=1, keepdims=True)
        whole = (GROUPS, 128)
        table[0] = jnp.broadcast_to(off0, whole)
        table[1] = jnp.broadcast_to(off1, whole)
        table[2] = jnp.broadcast_to((first < 128).astype(jnp.int32), whole)
        table[3] = jnp.broadcast_to(two.astype(jnp.int32), whole)
        to_smem = pltpu.make_async_copy(table, table_s, local_sem.at[CHUNKS + 1])
        to_smem.start()
        for s in range(CAP):
            for p in range(GROUPS // 2):
                pairs_out[s, p:p + 1, :] = jnp.where(
                    low, table[s, 2 * p:2 * p + 1, :], table[s, 2 * p + 1:2 * p + 2, :])
        to_smem.wait()
        proj_load.wait()

    def against(block, rows):
        return lax.dot_general(
            proj[block], rows, (((1,), (1,)), ((), ())), preferred_element_type=jnp.float32)

    def score(c, g):
        rows = gath[g, pl.ds(FIRST[c], ROWS), :]
        for s in range(CAP):
            first = pl.multiple_of(lax.rem(g, 2) * SLOTS + s * BLOCK, BLOCK)
            part_w[c, g // 2, pl.ds(first, BLOCK), :] = against(table_s[s, g, 0], rows)

    def score_pair(c, t):
        rows = gath[pl.ds(2 * t, 2), pl.ds(FIRST[c], 64), :].reshape(ROWS, gath.shape[2])
        for s in range(CAP):
            one = against(table_s[s, 2 * t, 0], rows)
            other = against(table_s[s, 2 * t + 1, 0], rows)
            part_h[c - WHOLE, t, s * BLOCK:(s + 1) * BLOCK, :] = jnp.where(low, one, other)

    def near(v):
        return v + v // 2

    def row_of(v):
        return lax.rem(y + v, SIDE)

    def scores_early(c):
        if c < WHOLE:
            @pl.loop(0, 9)
            def _(k):
                score(c, group(0, y + near(k // 3), z + near(lax.rem(k, 3))))
        else:
            @pl.loop(0, 3)
            def _(k):
                score_pair(c, 2 * row_of(near(k)) + z // 2)

    def scores_late(c):
        if c < WHOLE:
            @pl.loop(0, 4)
            def _(k):
                score(c, group(0, y + 2, z + k))

            @pl.loop(0, 3)
            def _(k):
                score(c, group(0, y + near(k), z + 2))
        else:
            @pl.loop(0, 3)
            def _(k):
                score_pair(c, 2 * row_of(near(k)) + 1 - z // 2)

            @pl.loop(0, 2)
            def _(k):
                score_pair(c, 2 * row_of(2) + k)

        for t in range(XS):
            send(part(c).at[2 * t + 1 - core], pair_in(c).at[t],
                 pair_send.at[c * XS + t], pair_recv.at[c * XS + t], {"pix": partner})

    def post_pair(c):
        for t in range(XS):
            at = c * XS + t
            arrived(pair_in(c).at[t], pair_send.at[at], pair_recv.at[at], {"pix": partner})
        for d in (2, 1, 3, 0):
            t = lax.rem(x + d, XS)
            mine = 2 * t + core
            part(c)[mine] = part(c)[mine] + pair_in(c)[t]
            if d:
                at = c * 3 + d - 1
                send(part(c).at[mine], x_in(c).at[d - 1], x_send.at[at], x_recv.at[at],
                     {"pix": mine})

    def units(c):
        return range(2 if c < WHOLE else 1)

    def filled(c, j):
        rows = []
        for s in range(CAP):
            one = table[2 + s, pl.ds(2 * pix + j, 1), :]
            if c >= WHOLE:
                one = jnp.where(low, one, table[2 + s, pl.ds(2 * pix + 1, 1), :])
            rows.append(one > 0)
        return rows

    def scaling_of(c, j):
        if c < WHOLE:
            return scales_all[2 * pix + j, c:c + 1, :]
        one = scales_all[2 * pix, 2:3, :]
        other = scales_all[2 * pix + 1, 2:3, :]
        if c == WHOLE:
            return jnp.where(low, one, pltpu.roll(other, 64, 1))
        return jnp.where(low, pltpu.roll(one, 64, 1), other)

    def post_stats(c):
        for d in (1, 2, 3):
            at = c * 3 + d - 1
            arrived(x_in(c).at[d - 1], x_send.at[at], x_recv.at[at],
                    {"pix": 2 * lax.rem(x + XS - d, XS) + core})
        for j in units(c):
            scaling = scaling_of(c, j)
            live = filled(c, j)
            peak = jnp.full((1, ROWS), -1e30, jnp.float32)
            for s in range(CAP):
                at = pl.ds(j * SLOTS + s * BLOCK, BLOCK)
                others = x_in(c)
                total = (part(c)[pix, at, :] + others[0, at, :]) + (others[1, at, :] + others[2, at, :])
                value = jnp.where(live[s], total * scaling, jnp.float32(-1e30))
                logit[c, at, :] = value
                peak = jnp.maximum(peak, jnp.max(value, axis=0, keepdims=True))
            run = jnp.zeros((1, ROWS), jnp.float32)
            for s in range(CAP):
                value = logit[c, pl.ds(j * SLOTS + s * BLOCK, BLOCK), :]
                value = jnp.where(live[s], jnp.exp(value - peak), 0.0)
                run = run + jnp.sum(value, axis=0, keepdims=True)
            stats[c, me, j:j + 1, :] = peak
            stats[c, me, 2 + j:3 + j, :] = run
        for k, peer in enumerate(img_peers):
            at = c * (GROUPS - 1) + k
            send(stats.at[c, me], stats.at[c, me], st_send.at[at], st_recv.at[at], {"img": peer})

    def weight_slot(c, p):
        return wts_w.at[c, pl.ds(2 * p, 2)] if c < WHOLE else wts_h.at[c - WHOLE, p]

    def post_weights(c):
        for k in range(GROUPS - 1):
            at = c * (GROUPS - 1) + k
            source = lax.rem(me + GROUPS - 1 - k, GROUPS)
            arrived(stats.at[c, source], st_send.at[at], st_recv.at[at], {"img": source})
        for j in units(c):
            live = filled(c, j)
            peaks = stats[c, :, j, :]
            peak = jnp.max(peaks, axis=0, keepdims=True)
            total = jnp.sum(stats[c, :, 2 + j, :] * jnp.exp(peaks - peak), axis=0, keepdims=True)
            row = 2 * j + c if c < WHOLE else 2 + c
            evid[pix, row:row + 1, :] = peak + jnp.log(total)
            inverse = 1.0 / total
            for s in range(CAP):
                value = logit[c, pl.ds(j * SLOTS + s * BLOCK, BLOCK), :]
                value = jnp.where(live[s], jnp.exp(value - peak) * inverse, 0.0).astype(jnp.bfloat16)
                if c < WHOLE:
                    wts_w[c, 2 * pix + j, s * BLOCK:(s + 1) * BLOCK, :] = value
                else:
                    wts_h[c - WHOLE, pix, s * BLOCK:(s + 1) * BLOCK, :] = value
        mine = weight_slot(c, pix)
        for d in (2, 1, 3):
            at = c * 7 + d
            send(mine, mine, w_send.at[at], w_recv.at[at],
                 {"pix": 2 * lax.rem(x + d, XS) + core})
        send(mine, mine, w_send.at[c * 7], w_recv.at[c * 7], {"pix": partner})

    def post_relay(c):
        for d in (1, 3, 2):
            source = 2 * lax.rem(x + XS - d, XS) + core
            ref = weight_slot(c, source)
            arrived(ref, w_send.at[c * 7 + d], w_recv.at[c * 7 + d], {"pix": source})
            send(ref, ref, w_send.at[c * 7 + 3 + d], w_recv.at[c * 7 + 3 + d], {"pix": partner})

    def post_weights_in(c):
        arrived(weight_slot(c, partner), w_send.at[c * 7], w_recv.at[c * 7], {"pix": partner})
        for d in (1, 3, 2):
            ref = weight_slot(c, 2 * lax.rem(x + XS - d, XS) + 1 - core)
            arrived(ref, w_send.at[c * 7 + 3 + d], w_recv.at[c * 7 + 3 + d], {"pix": partner})

    def place(c):
        @pl.loop(0, GROUPS)
        def _(g):
            columns = pl.ds(pl.multiple_of(g * ROWS, ROWS), ROWS)
            for b in range(proj.shape[0]):
                value = jnp.zeros((BLOCK, ROWS), jnp.bfloat16)
                for s in range(CAP):
                    value = value + jnp.where(
                        table_s[s, g, 0] == b, wts_w[c, g, s * BLOCK:(s + 1) * BLOCK, :], jnp.bfloat16(0))
                wfull[b * BLOCK:(b + 1) * BLOCK, columns] = value

    def add_images(c, lo, hi):
        @pl.loop(lo, hi)
        def _(u):
            rows = pl.ds(pl.multiple_of(lax.rem(u, 4) * SLOTS, SLOTS), SLOTS)
            columns = pl.ds(pl.multiple_of((u // 4) * COLS, COLS), COLS)
            there = gath[:, pl.ds(FIRST[c], ROWS), columns].reshape(GROUPS * ROWS, COLS)
            value = jnp.dot(wfull[rows, :], there, preferred_element_type=jnp.float32)
            acc[rows, columns] = value if c == 0 else acc[rows, columns] + value

    stores = []

    def store(src, dst):
        copy = pltpu.make_async_copy(src, dst, local_sem.at[CHUNKS + 2 + len(stores)])
        copy.start()
        stores.append(copy)

    def store_images(c):
        store(gath.at[:, pl.ds(FIRST[c], 64), :],
              late_images.at[:, pl.ds(FIRST[c] - FIRST[WHOLE], 64), :])

    p1_own(0)
    exchange_lists()
    stage1(0)
    build_table()

    stage2(0)
    p1_own(1)
    stage3(0, range(4))
    stage1(1)
    scores_early(0)
    stage4(0)
    scores_late(0)

    stage2(1)
    p1_own(2)
    post_pair(0)
    stage3(1, (0, 1))
    post_stats(0)
    stage3(1, (2, 3))
    stage1(2)
    post_weights(0)
    scores_early(1)
    stage4(1)
    post_relay(0)
    scores_late(1)

    stage2(2)
    p1_own(3)
    post_weights_in(0)
    place(0)
    post_pair(1)
    stage3(2, (0,))
    add_images(0, 0, 3)
    stage3(2, (1,))
    add_images(0, 3, 6)
    stage3(2, (2, 3))
    post_stats(1)
    stage1(3)
    scores_early(2)
    add_images(0, 6, 14)
    post_weights(1)
    stage4(2)
    scores_late(2)
    store_images(2)

    stage2(3)
    add_images(0, 14, 16)
    post_pair(2)
    stage3(3, (0, 1))
    post_relay(1)
    stage3(3, (2, 3))
    post_stats(2)
    post_weights_in(1)
    place(1)
    scores_early(3)
    post_weights(2)
    stage4(3)
    scores_late(3)
    store_images(3)

    add_images(1, 0, 4)
    post_pair(3)
    post_relay(2)
    add_images(1, 4, 12)
    post_stats(3)
    add_images(1, 12, 16)
    store(acc, early_sums)
    post_weights(3)
    for k, peer in enumerate(pix_peers):
        send(evid.at[pix], evid.at[pix], ev_send.at[k], ev_recv.at[k], {"pix": peer})
    post_relay(3)
    post_weights_in(2)
    post_weights_in(3)
    store(wts_h, late_weights)
    for k in range(2 * XS - 1):
        source = lax.rem(pix + 2 * XS - 1 - k, 2 * XS)
        arrived(evid.at[source], ev_send.at[k], ev_recv.at[k], {"pix": source})
    odd = lax.rem(me, 2)
    mine = evid[me // 2]
    for c in range(WHOLE):
        evidence_out[c:c + 1, :] = jnp.where(odd == 0, mine[c:c + 1], mine[2 + c:3 + c])
    third, fourth = mine[4:5], mine[5:6]
    evidence_out[WHOLE:WHOLE + 1, :] = jnp.where(
        odd == 0,
        jnp.where(low, third, pltpu.roll(fourth, 64, 1)),
        jnp.where(low, pltpu.roll(third, 64, 1), fourth),
    )
    for copy in drains:
        copy.wait_send()
    for copy in stores:
        copy.wait()


def gather_and_weigh(images, projections, ids, count, scales):
    rows, pixels = images.shape
    late = rows - FIRST[WHOLE]
    owned = projections.shape[0] * BLOCK
    dma = pltpu.SemaphoreType.DMA
    any_space = pl.BlockSpec(memory_space=pl.ANY)
    vmem = pl.BlockSpec(memory_space=pltpu.VMEM)
    n_img, n_pix = GROUPS - 1, 2 * XS - 1
    f32, bf16 = jnp.float32, jnp.bfloat16
    half = CHUNKS - WHOLE
    return pl.pallas_call(
        gather_kernel,
        out_shape=(
            jax.ShapeDtypeStruct((GROUPS, late, pixels), bf16),
            jax.ShapeDtypeStruct((half, 2 * XS, SLOTS, ROWS), bf16),
            jax.ShapeDtypeStruct((owned, pixels), f32),
            jax.ShapeDtypeStruct((CAP, GROUPS // 2, ROWS), jnp.int32),
            jax.ShapeDtypeStruct((3, 128), f32),
        ),
        in_specs=[any_space, any_space, vmem, pl.BlockSpec(memory_space=pltpu.SMEM), vmem],
        out_specs=(any_space, any_space, any_space, vmem, vmem),
        scratch_shapes=[
            pltpu.VMEM((GROUPS, rows, pixels), bf16),
            pltpu.VMEM(projections.shape, bf16),
            pltpu.VMEM((GROUPS, 8, 128), jnp.int32),
            pltpu.VMEM((GROUPS, 8, 128), f32),
            pltpu.VMEM((4, GROUPS, 128), jnp.int32),
            pltpu.SMEM((4, GROUPS, 128), jnp.int32),
            pltpu.VMEM((WHOLE, 2 * XS, 2 * SLOTS, ROWS), f32),
            pltpu.VMEM((half, 2 * XS, SLOTS, ROWS), f32),
            pltpu.VMEM((WHOLE, XS, 2 * SLOTS, ROWS), f32),
            pltpu.VMEM((half, XS, SLOTS, ROWS), f32),
            pltpu.VMEM((WHOLE, 3, 2 * SLOTS, ROWS), f32),
            pltpu.VMEM((half, 3, SLOTS, ROWS), f32),
            pltpu.VMEM((CHUNKS, 2 * SLOTS, ROWS), f32),
            pltpu.VMEM((CHUNKS, GROUPS, 8, ROWS), f32),
            pltpu.VMEM((WHOLE, GROUPS, SLOTS, ROWS), bf16),
            pltpu.VMEM((half, 2 * XS, SLOTS, ROWS), bf16),
            pltpu.VMEM((owned, GROUPS * ROWS), bf16),
            pltpu.VMEM((owned, pixels), f32),
            pltpu.VMEM((2 * XS, 8, 128), f32),
            dma((CHUNKS * 40,)), dma((CHUNKS * 40,)),
            dma((n_img,)), dma((n_img,)),
            dma((n_img,)), dma((n_img,)),
            dma((CHUNKS * XS,)), dma((CHUNKS * XS,)),
            dma((CHUNKS * 3,)), dma((CHUNKS * 3,)),
            dma((CHUNKS * n_img,)), dma((CHUNKS * n_img,)),
            dma((CHUNKS * 7,)), dma((CHUNKS * 7,)),
            dma((n_pix,)), dma((n_pix,)),
            dma((CHUNKS + 6,)),
        ],
        compiler_params=pltpu.CompilerParams(
            collective_id=0, has_side_effects=True, vmem_limit_bytes=63 * 1024 * 1024
        ),
        name="gather_and_weigh",
    )(images, projections, ids, count, scales)


def sum_kernel(pairs, early, images, weights, out, wfull):
    half = weights.shape[0]
    pair_count = weights.shape[1]
    depth = pair_count * ROWS

    @pl.when(pl.program_id(0) == 0)
    def _():
        for c in range(half):
            for p in range(pair_count):
                at = [pairs[s, p:p + 1, :] for s in range(CAP)]
                value = [weights[c, p, s * BLOCK:(s + 1) * BLOCK, :].astype(jnp.float32) for s in range(CAP)]
                for b in range(wfull.shape[0] // BLOCK):
                    placed = jnp.where(at[0] == b, value[0], 0.0) + jnp.where(at[1] == b, value[1], 0.0)
                    first = (c * pair_count + p) * ROWS
                    wfull[b * BLOCK:(b + 1) * BLOCK, first:first + ROWS] = placed.astype(jnp.bfloat16)

    there = [images[:, c * 64:(c + 1) * 64, :].reshape(depth, images.shape[2]) for c in range(half)]
    for m in range(wfull.shape[0] // SLOTS):
        rows = slice(m * SLOTS, (m + 1) * SLOTS)
        value = early[rows, :]
        for c in range(half):
            value = value + jnp.dot(
                wfull[rows, c * depth:(c + 1) * depth], there[c], preferred_element_type=jnp.float32)
        out[rows, :] = value


def sum_images(pairs, early, images, weights):
    owned, pixels = early.shape
    groups, late, _ = images.shape
    tile = 512
    return pl.pallas_call(
        sum_kernel,
        out_shape=jax.ShapeDtypeStruct((owned, pixels), jnp.float32),
        grid=(pixels // tile,),
        in_specs=[
            pl.BlockSpec(pairs.shape, lambda f: (0, 0, 0)),
            pl.BlockSpec((owned, tile), lambda f: (0, f)),
            pl.BlockSpec((groups, late, tile), lambda f: (0, 0, f)),
            pl.BlockSpec(weights.shape, lambda f: (0, 0, 0, 0)),
        ],
        out_specs=pl.BlockSpec((owned, tile), lambda f: (0, f)),
        scratch_shapes=[pltpu.VMEM((owned, groups * late), jnp.bfloat16)],
        compiler_params=pltpu.CompilerParams(
            dimension_semantics=("arbitrary",), vmem_limit_bytes=48 * 1024 * 1024
        ),
        name="sum_images",
    )(pairs, early, images, weights)


def on_device(images, inverse_noise_scale, projections, group_search_blocks, search_list_count):
    group_rows, pixels = images.shape
    share_rows = group_rows // lax.axis_size("pix")
    late_images, late_weights, early, pairs, evidence = gather_and_weigh(
        images, projections.reshape(-1, BLOCK, pixels), group_search_blocks, search_list_count,
        inverse_noise_scale.reshape(-1, ROWS),
    )
    sums = sum_images(pairs, early, late_images, late_weights)
    first_row = lax.axis_index("pix") * share_rows
    return sums, lax.dynamic_slice_in_dim(evidence.reshape(-1), first_row, share_rows)


def solution(mesh):
    placed = (P("img", "pix"), P("img"), P("img", "pix"), P("img", None), P("img"))
    return jax.shard_map(
        on_device,
        mesh=mesh,
        in_specs=placed,
        out_specs=(P("img", "pix"), P(("img", "pix"))),
        check_vma=False,
    )
```

```python
import functools

import jax
import jax.numpy as jnp
from jax import lax
from jax.experimental import pallas as pl
from jax.experimental.pallas import tpu as pltpu
from jax.sharding import PartitionSpec as P

BLOCK = 128
CAP = 2
MAXL = 16
SIDE = 4
GROUPS = SIDE * SIDE
XS = 4
FIRST = (0, 128, 256, 320)
SIZE = (128, 128, 64, 64)
CHUNKS = len(SIZE)
WHOLE = 2
ROWS = 128
COLS = 512
SLOTS = CAP * BLOCK
MESH = pl.DeviceIdType.MESH


def gather_kernel(
    images, projections, ids, count, scales,
    late_images, late_weights, early_sums, pairs_out, evidence_out,
    gath, proj, ids_all, scales_all, table, table_s, part_w, part_h, pair_w, pair_h, x_w, x_h,
    logit, stats, wts_w, wts_h, wfull, acc, evid,
    ag_send, ag_recv, id_send, id_recv, sc_send, sc_recv, pair_send, pair_recv, x_send, x_recv,
    st_send, st_recv, w_send, w_recv, ev_send, ev_recv, local_sem,
):
    me = lax.axis_index("img")
    pix = lax.axis_index("pix")
    y, z = me // SIDE, lax.rem(me, SIDE)
    x, core = pix // 2, lax.rem(pix, 2)
    partner = 2 * x + 1 - core
    drains = []
    lane = lax.broadcasted_iota(jnp.int32, (1, 128), 1)
    low = lane < 64

    def remote(src, dst, ssem, rsem, device):
        return pltpu.make_async_remote_copy(
            src_ref=src, dst_ref=dst, send_sem=ssem, recv_sem=rsem,
            device_id=device, device_id_type=MESH,
        )

    def send(src, dst, ssem, rsem, device):
        copy = remote(src, dst, ssem, rsem, device)
        copy.start()
        drains.append(copy)

    def arrived(ref, ssem, rsem, device):
        remote(ref, ref, ssem, rsem, device).wait_recv()

    img_peers = [lax.rem(me + k, GROUPS) for k in range(1, GROUPS)]
    pix_peers = [lax.rem(pix + k, 2 * XS) for k in range(1, 2 * XS)]

    def part(c):
        return part_w.at[c] if c < WHOLE else part_h.at[c - WHOLE]

    def pair_in(c):
        return pair_w.at[c] if c < WHOLE else pair_h.at[c - WHOLE]

    def x_in(c):
        return x_w.at[c] if c < WHOLE else x_h.at[c - WHOLE]

    loads = []
    for c in range(CHUNKS):
        rows = pl.ds(FIRST[c], SIZE[c])
        load = pltpu.make_async_copy(images.at[rows, :], gath.at[me, rows, :], local_sem.at[c])
        load.start()
        loads.append(load)
    proj_load = pltpu.make_async_copy(projections, proj, local_sem.at[CHUNKS])
    proj_load.start()
    ids_all[me, 0:1, 0:MAXL] = ids[...]
    ids_all[me, 1:2, :] = jnp.full((1, 128), count[0], jnp.int32)
    scales_all[me, 0:3, :] = scales[...]

    barrier = pltpu.get_barrier_semaphore()
    for peer in img_peers:
        pl.semaphore_signal(barrier, inc=1, device_id={"img": peer}, device_id_type=MESH)
    for peer in pix_peers:
        pl.semaphore_signal(barrier, inc=1, device_id={"pix": peer}, device_id_type=MESH)
    pl.semaphore_wait(barrier, len(img_peers) + len(pix_peers))

    def group(h, a, b):
        a, b = lax.rem(a + 2 * SIDE, SIDE), lax.rem(b + 2 * SIDE, SIDE)
        return a * SIDE + b if h == 0 else b * SIDE + a

    own = [(y, z), (z, y)]

    def slot(g, c, h, part_of=None):
        size = SIZE[c] // 2
        first = FIRST[c] + h * size
        if part_of is not None:
            size //= 2
            first += part_of * size
        return gath.at[g, pl.ds(first, size), :]

    def sems(c, h, k):
        at = (c * 2 + h) * 20 + k
        return ag_send.at[at], ag_recv.at[at]

    STEP = (1, -1)
    ORDER = (0, -1, 1, 2)

    def p1_own(c):
        loads[c].wait()
        for h in range(2):
            a, b = own[h]
            for k in range(2):
                ref = slot(me, c, h)
                send(ref, ref, *sems(c, h, k), {"img": group(h, a + STEP[k], b)})

    def p2_send(c, h, i):
        a, b = own[h]
        for k in range(2):
            ref = slot(group(h, a + ORDER[i], b), c, h)
            send(ref, ref, *sems(c, h, 4 + 2 * i + k), {"img": group(h, a, b + STEP[k])})

    def stage1(c):
        for h in range(2):
            p2_send(c, h, 0)
        for k in range(2):
            for h in range(2):
                a, b = own[h]
                g = group(h, a - STEP[k], b)
                arrived(slot(g, c, h), *sems(c, h, k), {"img": g})
                ref = slot(g, c, h, k)
                send(ref, ref, *sems(c, h, 2 + k), {"img": group(h, a + STEP[k], b)})
                p2_send(c, h, 1 + k)

    def stage2(c):
        for h in range(2):
            a, b = own[h]
            for k in range(2):
                arrived(
                    slot(group(h, a + 2, b), c, h, k), *sems(c, h, 2 + k),
                    {"img": group(h, a - STEP[k], b)},
                )
            p2_send(c, h, 3)

    def stage3(c, shards):
        for i in shards:
            for h in range(2):
                a, b = own[h]
                for k in range(2):
                    g = group(h, a + ORDER[i], b - STEP[k])
                    source = {"img": group(h, a, b - STEP[k])}
                    arrived(slot(g, c, h), *sems(c, h, 4 + 2 * i + k), source)
                    ref = slot(g, c, h, k)
                    send(ref, ref, *sems(c, h, 12 + 2 * i + k), {"img": group(h, a, b + STEP[k])})

    def stage4(c):
        for i in range(4):
            for h in range(2):
                a, b = own[h]
                for k in range(2):
                    arrived(
                        slot(group(h, a + ORDER[i], b + 2), c, h, k), *sems(c, h, 12 + 2 * i + k),
                        {"img": group(h, a, b - STEP[k])},
                    )

    def exchange_lists():
        for k, peer in enumerate(img_peers):
            send(ids_all.at[me], ids_all.at[me], id_send.at[k], id_recv.at[k], {"img": peer})
            send(scales_all.at[me], scales_all.at[me], sc_send.at[k], sc_recv.at[k], {"img": peer})

    def build_table():
        for k in range(GROUPS - 1):
            source = lax.rem(me + GROUPS - 1 - k, GROUPS)
            arrived(ids_all.at[source], id_send.at[k], id_recv.at[k], {"img": source})
            arrived(scales_all.at[source], sc_send.at[k], sc_recv.at[k], {"img": source})
        lists = ids_all[:, 0, :]
        counts = ids_all[:, 1, :]
        at = lax.broadcasted_iota(jnp.int32, (GROUPS, 128), 1)
        hit = (at < counts) & ((lists >> 3) == me) & (at < MAXL)
        first = jnp.min(jnp.where(hit, at, 128), axis=1, keepdims=True)
        last = jnp.max(jnp.where(hit, at, -1), axis=1, keepdims=True)
        two = last > first
        offset = lists & 7
        off0 = jnp.sum(jnp.where(at == first, offset, 0), axis=1, keepdims=True)
        off1 = jnp.sum(jnp.where((at == last) & two, offset, 0), axis=1, keepdims=True)
        whole = (GROUPS, 128)
        table[0] = jnp.broadcast_to(off0, whole)
        table[1] = jnp.broadcast_to(off1, whole)
        table[2] = jnp.broadcast_to((first < 128).astype(jnp.int32), whole)
        table[3] = jnp.broadcast_to(two.astype(jnp.int32), whole)
        to_smem = pltpu.make_async_copy(table, table_s, local_sem.at[CHUNKS + 1])
        to_smem.start()
        for s in range(CAP):
            for p in range(GROUPS // 2):
                pairs_out[s, p:p + 1, :] = jnp.where(
                    low, table[s, 2 * p:2 * p + 1, :], table[s, 2 * p + 1:2 * p + 2, :])
        to_smem.wait()
        proj_load.wait()

    def against(block, rows):
        return lax.dot_general(
            proj[block], rows, (((1,), (1,)), ((), ())), preferred_element_type=jnp.float32)

    def score(c, g):
        rows = gath[g, pl.ds(FIRST[c], ROWS), :]
        for s in range(CAP):
            first = pl.multiple_of(lax.rem(g, 2) * SLOTS + s * BLOCK, BLOCK)
            part_w[c, g // 2, pl.ds(first, BLOCK), :] = against(table_s[s, g, 0], rows)

    def score_pair(c, t):
        rows = gath[pl.ds(2 * t, 2), pl.ds(FIRST[c], 64), :].reshape(ROWS, gath.shape[2])
        for s in range(CAP):
            one = against(table_s[s, 2 * t, 0], rows)
            other = against(table_s[s, 2 * t + 1, 0], rows)
            part_h[c - WHOLE, t, s * BLOCK:(s + 1) * BLOCK, :] = jnp.where(low, one, other)

    def near(v):
        return v + v // 2

    def row_of(v):
        return lax.rem(y + v, SIDE)

    def scores_early(c):
        if c < WHOLE:
            @pl.loop(0, 9)
            def _(k):
                score(c, group(0, y + near(k // 3), z + near(lax.rem(k, 3))))
        else:
            @pl.loop(0, 3)
            def _(k):
                score_pair(c, 2 * row_of(near(k)) + z // 2)

    def scores_late(c):
        if c < WHOLE:
            @pl.loop(0, 4)
            def _(k):
                score(c, group(0, y + 2, z + k))

            @pl.loop(0, 3)
            def _(k):
                score(c, group(0, y + near(k), z + 2))
        else:
            @pl.loop(0, 3)
            def _(k):
                score_pair(c, 2 * row_of(near(k)) + 1 - z // 2)

            @pl.loop(0, 2)
            def _(k):
                score_pair(c, 2 * row_of(2) + k)

        for t in range(XS):
            send(part(c).at[2 * t + 1 - core], pair_in(c).at[t],
                 pair_send.at[c * XS + t], pair_recv.at[c * XS + t], {"pix": partner})

    def post_pair(c):
        for t in range(XS):
            at = c * XS + t
            arrived(pair_in(c).at[t], pair_send.at[at], pair_recv.at[at], {"pix": partner})
        for d in (2, 1, 3, 0):
            t = lax.rem(x + d, XS)
            mine = 2 * t + core
            part(c)[mine] = part(c)[mine] + pair_in(c)[t]
            if d:
                at = c * 3 + d - 1
                send(part(c).at[mine], x_in(c).at[d - 1], x_send.at[at], x_recv.at[at],
                     {"pix": mine})

    def units(c):
        return range(2 if c < WHOLE else 1)

    def filled(c, j):
        rows = []
        for s in range(CAP):
            one = table[2 + s, pl.ds(2 * pix + j, 1), :]
            if c >= WHOLE:
                one = jnp.where(low, one, table[2 + s, pl.ds(2 * pix + 1, 1), :])
            rows.append(one > 0)
        return rows

    def scaling_of(c, j):
        if c < WHOLE:
            return scales_all[2 * pix + j, c:c + 1, :]
        one = scales_all[2 * pix, 2:3, :]
        other = scales_all[2 * pix + 1, 2:3, :]
        if c == WHOLE:
            return jnp.where(low, one, pltpu.roll(other, 64, 1))
        return jnp.where(low, pltpu.roll(one, 64, 1), other)

    def post_stats(c):
        for d in (1, 2, 3):
            at = c * 3 + d - 1
            arrived(x_in(c).at[d - 1], x_send.at[at], x_recv.at[at],
                    {"pix": 2 * lax.rem(x + XS - d, XS) + core})
        for j in units(c):
            scaling = scaling_of(c, j)
            live = filled(c, j)
            peak = jnp.full((1, ROWS), -1e30, jnp.float32)
            for s in range(CAP):
                at = pl.ds(j * SLOTS + s * BLOCK, BLOCK)
                others = x_in(c)
                total = (part(c)[pix, at, :] + others[0, at, :]) + (others[1, at, :] + others[2, at, :])
                value = jnp.where(live[s], total * scaling, jnp.float32(-1e30))
                logit[c, at, :] = value
                peak = jnp.maximum(peak, jnp.max(value, axis=0, keepdims=True))
            run = jnp.zeros((1, ROWS), jnp.float32)
            for s in range(CAP):
                value = logit[c, pl.ds(j * SLOTS + s * BLOCK, BLOCK), :]
                value = jnp.where(live[s], jnp.exp(value - peak), 0.0)
                run = run + jnp.sum(value, axis=0, keepdims=True)
            stats[c, me, j:j + 1, :] = peak
            stats[c, me, 2 + j:3 + j, :] = run
        for k, peer in enumerate(img_peers):
            at = c * (GROUPS - 1) + k
            send(stats.at[c, me], stats.at[c, me], st_send.at[at], st_recv.at[at], {"img": peer})

    def weight_slot(c, p):
        return wts_w.at[c, pl.ds(2 * p, 2)] if c < WHOLE else wts_h.at[c - WHOLE, p]

    def post_weights(c):
        for k in range(GROUPS - 1):
            at = c * (GROUPS - 1) + k
            source = lax.rem(me + GROUPS - 1 - k, GROUPS)
            arrived(stats.at[c, source], st_send.at[at], st_recv.at[at], {"img": source})
        for j in units(c):
            live = filled(c, j)
            peaks = stats[c, :, j, :]
            peak = jnp.max(peaks, axis=0, keepdims=True)
            total = jnp.sum(stats[c, :, 2 + j, :] * jnp.exp(peaks - peak), axis=0, keepdims=True)
            row = 2 * j + c if c < WHOLE else 2 + c
            evid[pix, row:row + 1, :] = peak + jnp.log(total)
            inverse = 1.0 / total
            for s in range(CAP):
                value = logit[c, pl.ds(j * SLOTS + s * BLOCK, BLOCK), :]
                value = jnp.where(live[s], jnp.exp(value - peak) * inverse, 0.0).astype(jnp.bfloat16)
                if c < WHOLE:
                    wts_w[c, 2 * pix + j, s * BLOCK:(s + 1) * BLOCK, :] = value
                else:
                    wts_h[c - WHOLE, pix, s * BLOCK:(s + 1) * BLOCK, :] = value
        mine = weight_slot(c, pix)
        for d in (2, 1, 3):
            at = c * 7 + d
            send(mine, mine, w_send.at[at], w_recv.at[at],
                 {"pix": 2 * lax.rem(x + d, XS) + core})
        send(mine, mine, w_send.at[c * 7], w_recv.at[c * 7], {"pix": partner})

    def post_relay(c):
        for d in (1, 3, 2):
            source = 2 * lax.rem(x + XS - d, XS) + core
            ref = weight_slot(c, source)
            arrived(ref, w_send.at[c * 7 + d], w_recv.at[c * 7 + d], {"pix": source})
            send(ref, ref, w_send.at[c * 7 + 3 + d], w_recv.at[c * 7 + 3 + d], {"pix": partner})

    def post_weights_in(c):
        arrived(weight_slot(c, partner), w_send.at[c * 7], w_recv.at[c * 7], {"pix": partner})
        for d in (1, 3, 2):
            ref = weight_slot(c, 2 * lax.rem(x + XS - d, XS) + 1 - core)
            arrived(ref, w_send.at[c * 7 + 3 + d], w_recv.at[c * 7 + 3 + d], {"pix": partner})

    def place(c):
        @pl.loop(0, GROUPS)
        def _(g):
            columns = pl.ds(pl.multiple_of(g * ROWS, ROWS), ROWS)
            for b in range(proj.shape[0]):
                value = jnp.zeros((BLOCK, ROWS), jnp.bfloat16)
                for s in range(CAP):
                    value = value + jnp.where(
                        table_s[s, g, 0] == b, wts_w[c, g, s * BLOCK:(s + 1) * BLOCK, :], jnp.bfloat16(0))
                wfull[b * BLOCK:(b + 1) * BLOCK, columns] = value

    def add_images(c, lo, hi):
        @pl.loop(lo, hi)
        def _(u):
            rows = pl.ds(pl.multiple_of(lax.rem(u, 4) * SLOTS, SLOTS), SLOTS)
            columns = pl.ds(pl.multiple_of((u // 4) * COLS, COLS), COLS)
            there = gath[:, pl.ds(FIRST[c], ROWS), columns].reshape(GROUPS * ROWS, COLS)
            value = jnp.dot(wfull[rows, :], there, preferred_element_type=jnp.float32)
            acc[rows, columns] = value if c == 0 else acc[rows, columns] + value

    stores = []

    def store(src, dst):
        copy = pltpu.make_async_copy(src, dst, local_sem.at[CHUNKS + 2 + len(stores)])
        copy.start()
        stores.append(copy)

    def store_images(c):
        store(gath.at[:, pl.ds(FIRST[c], 64), :],
              late_images.at[:, pl.ds(FIRST[c] - FIRST[WHOLE], 64), :])

    p1_own(0)
    exchange_lists()
    stage1(0)
    build_table()

    stage2(0)
    p1_own(1)
    stage3(0, range(4))
    stage1(1)
    scores_early(0)
    stage4(0)
    scores_late(0)

    stage2(1)
    p1_own(2)
    post_pair(0)
    stage3(1, (0, 1))
    post_stats(0)
    stage3(1, (2, 3))
    stage1(2)
    post_weights(0)
    scores_early(1)
    stage4(1)
    post_relay(0)
    scores_late(1)

    stage2(2)
    p1_own(3)
    post_pair(1)
    post_weights_in(0)
    place(0)
    stage3(2, (0,))
    add_images(0, 0, 3)
    stage3(2, (1,))
    add_images(0, 3, 6)
    stage3(2, (2, 3))
    post_stats(1)
    stage1(3)
    scores_early(2)
    add_images(0, 6, 14)
    post_weights(1)
    stage4(2)
    scores_late(2)
    store_images(2)

    stage2(3)
    add_images(0, 14, 16)
    post_pair(2)
    stage3(3, (0, 1))
    post_relay(1)
    stage3(3, (2, 3))
    post_stats(2)
    post_weights_in(1)
    place(1)
    scores_early(3)
    post_weights(2)
    stage4(3)
    scores_late(3)
    store_images(3)

    add_images(1, 0, 4)
    post_pair(3)
    post_relay(2)
    add_images(1, 4, 12)
    post_stats(3)
    add_images(1, 12, 16)
    store(acc, early_sums)
    post_weights(3)
    for k, peer in enumerate(pix_peers):
        send(evid.at[pix], evid.at[pix], ev_send.at[k], ev_recv.at[k], {"pix": peer})
    post_relay(3)
    post_weights_in(2)
    post_weights_in(3)
    store(wts_h, late_weights)
    for k in range(2 * XS - 1):
        source = lax.rem(pix + 2 * XS - 1 - k, 2 * XS)
        arrived(evid.at[source], ev_send.at[k], ev_recv.at[k], {"pix": source})
    odd = lax.rem(me, 2)
    mine = evid[me // 2]
    for c in range(WHOLE):
        evidence_out[c:c + 1, :] = jnp.where(odd == 0, mine[c:c + 1], mine[2 + c:3 + c])
    third, fourth = mine[4:5], mine[5:6]
    evidence_out[WHOLE:WHOLE + 1, :] = jnp.where(
        odd == 0,
        jnp.where(low, third, pltpu.roll(fourth, 64, 1)),
        jnp.where(low, pltpu.roll(third, 64, 1), fourth),
    )
    for copy in drains:
        copy.wait_send()
    for copy in stores:
        copy.wait()


def gather_and_weigh(images, projections, ids, count, scales):
    rows, pixels = images.shape
    late = rows - FIRST[WHOLE]
    owned = projections.shape[0] * BLOCK
    dma = pltpu.SemaphoreType.DMA
    any_space = pl.BlockSpec(memory_space=pl.ANY)
    vmem = pl.BlockSpec(memory_space=pltpu.VMEM)
    n_img, n_pix = GROUPS - 1, 2 * XS - 1
    f32, bf16 = jnp.float32, jnp.bfloat16
    half = CHUNKS - WHOLE
    return pl.pallas_call(
        gather_kernel,
        out_shape=(
            jax.ShapeDtypeStruct((GROUPS, late, pixels), bf16),
            jax.ShapeDtypeStruct((half, 2 * XS, SLOTS, ROWS), bf16),
            jax.ShapeDtypeStruct((owned, pixels), f32),
            jax.ShapeDtypeStruct((CAP, GROUPS // 2, ROWS), jnp.int32),
            jax.ShapeDtypeStruct((3, 128), f32),
        ),
        in_specs=[any_space, any_space, vmem, pl.BlockSpec(memory_space=pltpu.SMEM), vmem],
        out_specs=(any_space, any_space, any_space, vmem, vmem),
        scratch_shapes=[
            pltpu.VMEM((GROUPS, rows, pixels), bf16),
            pltpu.VMEM(projections.shape, bf16),
            pltpu.VMEM((GROUPS, 8, 128), jnp.int32),
            pltpu.VMEM((GROUPS, 8, 128), f32),
            pltpu.VMEM((4, GROUPS, 128), jnp.int32),
            pltpu.SMEM((4, GROUPS, 128), jnp.int32),
            pltpu.VMEM((WHOLE, 2 * XS, 2 * SLOTS, ROWS), f32),
            pltpu.VMEM((half, 2 * XS, SLOTS, ROWS), f32),
            pltpu.VMEM((WHOLE, XS, 2 * SLOTS, ROWS), f32),
            pltpu.VMEM((half, XS, SLOTS, ROWS), f32),
            pltpu.VMEM((WHOLE, 3, 2 * SLOTS, ROWS), f32),
            pltpu.VMEM((half, 3, SLOTS, ROWS), f32),
            pltpu.VMEM((CHUNKS, 2 * SLOTS, ROWS), f32),
            pltpu.VMEM((CHUNKS, GROUPS, 8, ROWS), f32),
            pltpu.VMEM((WHOLE, GROUPS, SLOTS, ROWS), bf16),
            pltpu.VMEM((half, 2 * XS, SLOTS, ROWS), bf16),
            pltpu.VMEM((owned, GROUPS * ROWS), bf16),
            pltpu.VMEM((owned, pixels), f32),
            pltpu.VMEM((2 * XS, 8, 128), f32),
            dma((CHUNKS * 40,)), dma((CHUNKS * 40,)),
            dma((n_img,)), dma((n_img,)),
            dma((n_img,)), dma((n_img,)),
            dma((CHUNKS * XS,)), dma((CHUNKS * XS,)),
            dma((CHUNKS * 3,)), dma((CHUNKS * 3,)),
            dma((CHUNKS * n_img,)), dma((CHUNKS * n_img,)),
            dma((CHUNKS * 7,)), dma((CHUNKS * 7,)),
            dma((n_pix,)), dma((n_pix,)),
            dma((CHUNKS + 6,)),
        ],
        compiler_params=pltpu.CompilerParams(
            collective_id=0, has_side_effects=True, vmem_limit_bytes=63 * 1024 * 1024
        ),
        name="gather_and_weigh",
    )(images, projections, ids, count, scales)


def sum_kernel(pairs, early, images, weights, out, wfull):
    half = weights.shape[0]
    pair_count = weights.shape[1]
    depth = pair_count * ROWS

    @pl.when(pl.program_id(0) == 0)
    def _():
        for c in range(half):
            for p in range(pair_count):
                at = [pairs[s, p:p + 1, :] for s in range(CAP)]
                value = [weights[c, p, s * BLOCK:(s + 1) * BLOCK, :].astype(jnp.float32) for s in range(CAP)]
                for b in range(wfull.shape[0] // BLOCK):
                    placed = jnp.where(at[0] == b, value[0], 0.0) + jnp.where(at[1] == b, value[1], 0.0)
                    first = (c * pair_count + p) * ROWS
                    wfull[b * BLOCK:(b + 1) * BLOCK, first:first + ROWS] = placed.astype(jnp.bfloat16)

    there = [images[:, c * 64:(c + 1) * 64, :].reshape(depth, images.shape[2]) for c in range(half)]
    for m in range(wfull.shape[0] // SLOTS):
        rows = slice(m * SLOTS, (m + 1) * SLOTS)
        value = early[rows, :]
        for c in range(half):
            value = value + jnp.dot(
                wfull[rows, c * depth:(c + 1) * depth], there[c], preferred_element_type=jnp.float32)
        out[rows, :] = value


def sum_images(pairs, early, images, weights):
    owned, pixels = early.shape
    groups, late, _ = images.shape
    tile = 512
    return pl.pallas_call(
        sum_kernel,
        out_shape=jax.ShapeDtypeStruct((owned, pixels), jnp.float32),
        grid=(pixels // tile,),
        in_specs=[
            pl.BlockSpec(pairs.shape, lambda f: (0, 0, 0)),
            pl.BlockSpec((owned, tile), lambda f: (0, f)),
            pl.BlockSpec((groups, late, tile), lambda f: (0, 0, f)),
            pl.BlockSpec(weights.shape, lambda f: (0, 0, 0, 0)),
        ],
        out_specs=pl.BlockSpec((owned, tile), lambda f: (0, f)),
        scratch_shapes=[pltpu.VMEM((owned, groups * late), jnp.bfloat16)],
        compiler_params=pltpu.CompilerParams(
            dimension_semantics=("arbitrary",), vmem_limit_bytes=48 * 1024 * 1024
        ),
        name="sum_images",
    )(pairs, early, images, weights)


def on_device(images, inverse_noise_scale, projections, group_search_blocks, search_list_count):
    group_rows, pixels = images.shape
    share_rows = group_rows // lax.axis_size("pix")
    late_images, late_weights, early, pairs, evidence = gather_and_weigh(
        images, projections.reshape(-1, BLOCK, pixels), group_search_blocks, search_list_count,
        inverse_noise_scale.reshape(-1, ROWS),
    )
    sums = sum_images(pairs, early, late_images, late_weights)
    first_row = lax.axis_index("pix") * share_rows
    return sums, lax.dynamic_slice_in_dim(evidence.reshape(-1), first_row, share_rows)


def solution(mesh):
    placed = (P("img", "pix"), P("img"), P("img", "pix"), P("img", None), P("img"))
    return jax.shard_map(
        on_device,
        mesh=mesh,
        in_specs=placed,
        out_specs=(P("img", "pix"), P(("img", "pix"))),
        check_vma=False,
    )
```
